32 devices in a mesh: rows: 8 (over z, y), grp: 4 (over x, core).
Axes of the slice: x: 2, y: 2, z: 4, core: 2. Of those that a mesh axis runs over, the one named last changes fastest.
Arguments:
- modes: float32 [393216, 256], P(('rows', 'grp')), may hold values from -6 to 6
- points: int32 [196], replicated, may hold values from 0 to 393215, as said below
Outputs:
- residual: float32 [393216, 128], P(('rows', 'grp'))
- norms: float32 [4, 128], replicated
The draws below stay inside these ranges and needn't reach their ends.
Inputs may be any that keep to these rules, and one draw needn't show every extreme that they name: `points`: distinct row indices of the mode matrix.
All inputs are finite; a program needn't handle non-finite values.
Results may differ from the reference program's by a relative error of at most 0.00029.
Values sent between devices are 32-bit elements; how exact they have to be, the bound alone decides.
A program may use at most 128 MiB of HBM per device.

```python
import jax
import jax.numpy as jnp
from jax import lax

MODES = 256
FIT = 128
ROWS_DEV = 12288
PRIOR = 192
STEPS = 4
NPTS = 196
ROWS = 393216
N_ROWS = 8
N_GRP = 4


def draw_points(key, part):
    total = ROWS_DEV * N_ROWS * N_GRP
    order = jax.random.permutation(jax.random.fold_in(key, 11), total)
    return order[:NPTS].astype(jnp.int32)


def level_of(own_key, extent, shards, least, largest):
    level, own = 1.0, jax.random.fold_in(own_key, 6)
    for position, blocks in shards:
        heights = jnp.exp(jax.random.uniform(jax.random.fold_in(own, position), (blocks,), jnp.float32, least / len(shards), largest / len(shards)))
        level = level * jnp.repeat(heights, extent[position] // blocks).reshape([-1 if axis == position else 1 for axis in range(len(extent))])
    return level


def gaussian(own_key, shape, spread, bound, split=(), kind=jnp.bfloat16):
    factor_of = level_of(own_key, shape, split, -0.22, 0.18) if split else 1.0
    result = jax.random.normal(own_key, shape, jnp.float32) * spread * factor_of
    return jnp.minimum(jnp.maximum(result, -bound), bound).astype(kind)


def setup_inputs(seed: int = 0) -> dict:
    seeds = jax.random.split(jax.random.key(seed), 3)
    modes = gaussian(seeds[0], (ROWS, MODES), 1.0, 6.0, ((0, 32),), jnp.float32)
    points = draw_points(jax.random.fold_in(seeds[2], 71), 0)
    return {"modes": modes, "points": points}


def reference(modes, points):
    high = lax.Precision.HIGHEST
    sampled = modes[points.astype(jnp.int32)]
    fit_modes = modes[:, :FIT]
    rest_modes = modes[:, FIT:]
    total = ROWS_DEV * N_ROWS * N_GRP
    collected = []
    residual = rest_modes
    for step in range(STEPS):
        chosen = sampled[:PRIOR + step + 1]
        left = chosen[:, :FIT]
        right = chosen[:, FIT:]
        gram = jnp.dot(left.T.astype(jnp.float32), left.astype(jnp.float32), preferred_element_type=jnp.float32, precision=high)
        cross = jnp.dot(left.T.astype(jnp.float32), right.astype(jnp.float32), preferred_element_type=jnp.float32, precision=high)
        factor = jnp.linalg.cholesky(gram)
        coef = jax.scipy.linalg.cho_solve((factor, True), cross)
        residual = rest_modes - jnp.dot(fit_modes.astype(jnp.float32), coef.astype(jnp.float32), preferred_element_type=jnp.float32, precision=high)
        collected.append(jnp.sum(residual * residual, axis=0) / total)
    return (residual, jnp.stack(collected))
```

```python
import functools

import jax
import jax.numpy as jnp
from jax import lax
from jax.experimental import pallas as pl
from jax.experimental.pallas import tpu as pltpu
from jax.sharding import PartitionSpec as P

PRIOR = 192
BLOCK = 8
HIGH = lax.Precision.HIGHEST
MESH = pl.DeviceIdType.MESH
F32 = jnp.float32
BF16 = jnp.bfloat16


def dot(a, b, dims=((1,), (0,))):
    return lax.dot_general(a, b, (dims, ((), ())), precision=HIGH, preferred_element_type=F32)


def halves(value):
    hi = value.astype(BF16)
    return hi, (value - hi.astype(F32)).astype(BF16)


def flat_index(axes):
    (first, _), (second, width) = axes
    return lax.axis_index(first) * width + lax.axis_index(second)


def coords(axes, flat):
    width = axes[1][1]
    return (flat // width, lax.rem(flat, width))


def small_inverse(e):
    size = len(e)
    e = [list(line) for line in e]
    for p in range(size):
        inv = 1.0 / e[p][p]
        line = [e[p][j] * inv for j in range(size)]
        line[p] = -inv
        for i in range(size):
            for j in range(i, size):
                if i == p or j == p:
                    continue
                e[i][j] = e[i][j] - e[p][i] * line[j]
                e[j][i] = e[i][j]
        for j in range(size):
            e[p][j] = line[j]
            e[j][p] = line[j]
    return [[-value for value in line] for line in e]


def sweep_inverse(gram, width=BLOCK):
    size = gram.shape[0]
    shape = (8, size)
    tiles = [gram[8 * t : 8 * t + 8, :] for t in range(size // 8)]
    lane = lax.broadcasted_iota(jnp.int32, shape, 1)
    sub = lax.broadcasted_iota(jnp.int32, shape, 0)
    for k in range(0, size, width):
        t, s = k // 8, k % 8
        inside = (lane >= k) & (lane < k + width)
        own = [jnp.broadcast_to(tiles[t][:, k + q : k + q + 1], shape) for q in range(width)]
        entry = [[None] * width for _ in range(width)]
        for p in range(width):
            for q in range(p, width):
                entry[p][q] = jnp.broadcast_to(own[q][s + p : s + p + 1, :], shape)
                entry[q][p] = entry[p][q]
        small = small_inverse(entry)
        rows = []
        for q in range(width):
            row = jnp.broadcast_to(tiles[t][s + q : s + q + 1, :], shape)
            rows.append(jnp.where(inside, jnp.where(lane == k + q, -1.0, 0.0), row))
        scaled = []
        for p in range(width):
            line = small[p][0] * rows[0]
            for q in range(1, width):
                line = line + small[p][q] * rows[q]
            scaled.append(line)
        fresh = []
        for r in range(size // 8):
            value = jnp.where(inside, 0.0, tiles[r])
            for p in range(width):
                col = own[p] if r == t else jnp.broadcast_to(tiles[r][:, k + p : k + p + 1], shape)
                value = value - col * scaled[p]
            fresh.append(value)
        for p in range(width):
            fresh[t] = jnp.where(sub == s + p, scaled[p], fresh[t])
        tiles = fresh
    return -jnp.concatenate(tiles, axis=0)


def reducers_of(n, tiles):
    count = min(tiles, n // 2)
    return count, n // 4, (n // 2) // count


def solve_kernel(
    axes, n, points_hbm, modes_ref, held, pair, wide_ref, kept_ref, stat_ref,
    points_ref, listed, picked, acc, squares, part1, landed1, own1, full1, part2, landed2, own2, full2,
    local, send1, recv1, share1, gather1, send2, recv2, share2, gather2,
):
    me = flat_index(axes)
    rows_dev, cols = held.shape
    split = cols // 2
    npts = points_ref.shape[0]
    chunks = local.shape[0]
    rows = rows_dev // chunks
    count, first, stride = reducers_of(n, split // 8)
    deep = split // count
    mine = (me - first) // stride
    reduces = (me >= first) & (me < first + count * stride) & (lax.rem(me - first + n, stride) == 0)

    def fetch(c):
        return pltpu.make_async_copy(
            modes_ref.at[pl.ds(c * rows, rows), :], held.at[pl.ds(c * rows, rows), :], local.at[c]
        )

    def loop(body, start, stop):
        def step(i, carry):
            body(i)
            return carry

        lax.fori_loop(start, stop, step, 0)

    points_copy = pltpu.make_async_copy(points_hbm, points_ref, listed)
    points_copy.start()
    loop(lambda c: fetch(c).start(), 0, chunks)
    barrier = pltpu.get_barrier_semaphore()

    def greet(off):
        peer = lax.rem(me + off, n)
        pl.semaphore_signal(barrier, inc=1, device_id=coords(axes, peer), device_id_type=MESH)

    loop(greet, 1, n)
    acc[...] = jnp.zeros_like(acc)
    squares[...] = jnp.zeros_like(squares)

    def grams(c):
        fetch(c).wait()
        at = pl.ds(c * rows, rows)
        fit = held[at, :split]
        rest = held[at, split:]
        f_hi, f_lo = halves(fit)
        r_hi, r_lo = halves(rest)
        pair[at, :split] = f_hi
        pair[at, split:] = f_lo
        left = jnp.concatenate([f_hi, f_lo, r_lo], axis=1)
        right = jnp.concatenate([f_hi, r_hi], axis=1)
        acc[...] += lax.dot_general(left, right, (((0,), (0,)), ((), ())), preferred_element_type=F32)
        squares[...] += jnp.sum((rest * rest).reshape(-1, 8, split), axis=0)

    loop(grams, 0, chunks)

    points_copy.wait()
    base = me * rows_dev

    def take(i):
        at = points_ref[i] - base
        owned = (at >= 0) & (at < rows_dev)
        row = held[pl.ds(jnp.clip(at, 0, rows_dev - 1), 1), :]
        return jnp.where(owned, row, 0.0)

    def pick(t):
        for s in range(8):
            picked[pl.ds(t * 8 + s, 1), :] = take(t * 8 + s)

    picked[...] = jnp.zeros_like(picked)
    loop(pick, 0, npts // 8)
    for i in range(npts // 8 * 8, npts):
        picked[i : i + 1, :] = take(i)
    block = picked[...]
    index = lax.broadcasted_iota(jnp.int32, block.shape, 0)
    chosen = jnp.where(index <= PRIOR, block, 0.0)
    both = dot(chosen[:, :split], chosen, ((0,), (0,)))
    part1[...] = both[:, :split].reshape(part1.shape)

    def peer_copy(src, dst, sent, got, peer):
        return pltpu.make_async_remote_copy(
            src_ref=src, dst_ref=dst, send_sem=sent, recv_sem=got,
            device_id=coords(axes, peer), device_id_type=MESH,
        )

    def scatter(part, landed, sent, got):
        def body(off):
            i = lax.rem(me + off, count)
            peer = first + i * stride

            @pl.when(peer != me)
            def _():
                peer_copy(part.at[i], landed.at[me], sent, got, peer).start()

        loop(body, 0, count)

    def reduce(part, landed, own, full, got, shared, gathered):
        @pl.when(reduces)
        def _():
            seen = landed.at[pl.ds(0, n - 1)]
            peer_copy(seen, seen, shared, got, me).wait_recv()
            landed[me] = part[mine]
            total = landed[0]
            for j in range(1, n):
                total = total + landed[j]
            own[...] = total
            full[mine] = total

            def body(off):
                peer = lax.rem(me + off, n)
                peer_copy(own, full.at[mine], shared, gathered, peer).start()

            loop(body, 1, n)

    def collect(full, shared, gathered):
        for held_here, size in ((reduces, count - 1), (jnp.logical_not(reduces), count)):

            @pl.when(held_here)
            def _():
                seen = full.at[pl.ds(0, size)]
                peer_copy(seen, seen, shared, gathered, me).wait_recv()

    def drain(part, landed, sent, shared):
        for held_here, size in ((reduces, count - 1), (jnp.logical_not(reduces), count)):

            @pl.when(held_here)
            def _():
                seen = part.at[pl.ds(0, size)]
                peer_copy(seen, seen, sent, shared, me).wait_send()

        @pl.when(reduces)
        def _():
            seen = landed.at[pl.ds(0, n - 1)]
            peer_copy(seen, seen, shared, sent, me).wait_send()

    pl.semaphore_wait(barrier, n - 1)
    scatter(part1, landed1, send1, recv1)

    fold = acc[split : 2 * split, :split]
    ftf = acc[:split, :split] + (fold + fold.T)
    ftr = acc[:split, split:] + (acc[split : 2 * split, split:] + acc[2 * split :, :split].T)
    part2[...] = jnp.zeros_like(part2)
    part2[:, 0:deep, :] = both[:, split:].reshape(count, deep, split)
    part2[:, deep : 2 * deep, :] = ftf.reshape(count, deep, split)
    part2[:, 2 * deep : 3 * deep, :] = ftr.reshape(count, deep, split)
    fresh = npts - PRIOR - 1
    tail = slice(3 * deep, 3 * deep + 1)
    for i in range(fresh):
        for half in range(2):
            at = PRIOR + 1 + i
            part2[2 * i + half, tail, :] = picked[at : at + 1, half * split : (half + 1) * split]
    part2[2 * fresh, tail, :] = jnp.sum(squares[...], axis=0, keepdims=True)
    scatter(part2, landed2, send2, recv2)

    reduce(part1, landed1, own1, full1, recv1, share1, gather1)
    reduce(part2, landed2, own2, full2, recv2, share2, gather2)
    collect(full1, share1, gather1)
    gram = full1[...].reshape(split, split)
    inverse = sweep_inverse(gram)
    collect(full2, share2, gather2)
    cross = full2[:, 0:deep, :].reshape(split, split)
    coef = dot(inverse, cross)
    coef = coef + dot(inverse, cross - dot(gram, coef))
    left = [full2[2 * i, tail, :] for i in range(fresh)]
    right = [full2[2 * i + 1, tail, :] for i in range(fresh)]
    lefts = jnp.concatenate(left + [jnp.zeros((8 - fresh, split), F32)], axis=0)
    gains = dot(lefts, inverse)
    errors = dot(lefts, coef)
    ks, ss, ds = [], [], []
    kept = [coef]
    pad7 = jnp.zeros((7, split), F32)
    for j in range(fresh):
        k = gains[j : j + 1, :]
        d = right[j] - errors[j : j + 1, :]
        for k0, s0, d0 in zip(ks, ss, ds):
            along = jnp.sum(k0 * left[j], axis=1, keepdims=True)
            k = k - k0 * (along / s0)
            d = d - along * d0
        s = 1.0 + jnp.sum(k * left[j], axis=1, keepdims=True)
        d = d / s
        ks.append(k)
        ss.append(s)
        ds.append(d)
        turn = dot(jnp.concatenate([k, pad7], axis=0), jnp.concatenate([d, pad7], axis=0), ((0,), (0,)))
        kept.append(kept[-1] + turn)
    c_hi, c_lo = halves(kept[-1])
    wide_ref[0:split, 0:split] = c_hi
    wide_ref[split:, 0:split] = c_hi
    wide_ref[0:split, split:] = c_lo
    wide_ref[split:, split:] = jnp.zeros((split, split), BF16)
    kept_ref[...] = jnp.concatenate(kept, axis=1)
    stat_ref[0:split, 0:split] = full2[:, deep : 2 * deep, :].reshape(split, split)
    stat_ref[0:split, split:] = full2[:, 2 * deep : 3 * deep, :].reshape(split, split)
    stat_ref[split:, 0:split] = jnp.broadcast_to(full2[2 * fresh, tail, :], (8, split))
    stat_ref[split:, split:] = jnp.zeros((8, split), F32)
    drain(part1, landed1, send1, share1)
    drain(part2, landed2, send2, share2)


def residual_kernel(total_rows, held, pair, wide_ref, kept_ref, stat_ref, res_ref, norm_ref, made_buf, wrote):
    chunks, rows, split = made_buf.shape
    steps = norm_ref.shape[0]
    piece = 256 if rows % 256 == 0 else rows

    def flush(c):
        return pltpu.make_async_copy(made_buf.at[c], res_ref.at[pl.ds(c * rows, rows), :], wrote.at[c])

    wide = wide_ref[...]
    for c in range(chunks):
        for at in range(0, rows, piece):
            here = slice(c * rows + at, c * rows + at + piece)
            made = jnp.dot(pair[here, :], wide, preferred_element_type=F32)
            made_buf[c, at : at + piece, :] = held[here, split:] - (made[:, :split] + made[:, split:])
        flush(c).start()
    ftf, ftr = stat_ref[0:split, 0:split], stat_ref[0:split, split:]
    sq = stat_ref[split : split + 1, 0:split]
    curved = dot(ftf, kept_ref[...])
    for j in range(steps):
        cut = slice(j * split, (j + 1) * split)
        bent = kept_ref[:, cut] * (curved[:, cut] - 2.0 * ftr)
        norm_ref[j : j + 1, :] = (sq + jnp.sum(bent, axis=0, keepdims=True)) / total_rows
    for c in range(chunks):
        flush(c).wait()


def on_device(axes, modes, points):
    n = axes[0][1] * axes[1][1]
    rows_dev, cols = modes.shape
    split = cols // 2
    npts = points.shape[0]
    steps = npts - PRIOR
    padded = -(-npts // 8) * 8
    count, _, _ = reducers_of(n, split // 8)
    deep = split // count
    vmem = pl.BlockSpec(memory_space=pltpu.VMEM)
    any_space = pl.BlockSpec(memory_space=pl.ANY)
    chunks = 12 if rows_dev % 96 == 0 else 1

    def buffers(depth):
        return [
            pltpu.VMEM((count, depth, split), F32),
            pltpu.VMEM((n, depth, split), F32),
            pltpu.VMEM((depth, split), F32),
            pltpu.VMEM((count, depth, split), F32),
        ]

    held, pair, wide, kept, stat = pl.pallas_call(
        functools.partial(solve_kernel, axes, n),
        out_shape=[
            pltpu.VMEM((rows_dev, cols), F32),
            pltpu.VMEM((rows_dev, cols), BF16),
            pltpu.VMEM((cols, cols), BF16),
            pltpu.VMEM((split, steps * split), F32),
            pltpu.VMEM((split + 8, cols), F32),
        ],
        in_specs=[pl.BlockSpec(memory_space=pltpu.HBM)] * 2,
        out_specs=[vmem] * 5,
        scratch_shapes=[
            pltpu.SMEM((npts,), jnp.int32),
            pltpu.SemaphoreType.DMA,
            pltpu.VMEM((padded, cols), F32),
            pltpu.VMEM((3 * split, cols), F32),
            pltpu.VMEM((8, split), F32),
        ]
        + buffers(deep)
        + buffers(3 * deep + 1)
        + [pltpu.SemaphoreType.DMA((chunks,))]
        + [pltpu.SemaphoreType.DMA] * 8,
        compiler_params=pltpu.CompilerParams(
            collective_id=0, has_side_effects=True, vmem_limit_bytes=16 * 1024 * 1024
        ),
        name="solve",
    )(pltpu.with_memory_space_constraint(points, pltpu.HBM), pltpu.with_memory_space_constraint(modes, pltpu.HBM))
    residual, norms = pl.pallas_call(
        functools.partial(residual_kernel, rows_dev * n),
        out_shape=[
            jax.ShapeDtypeStruct((rows_dev, split), F32),
            jax.ShapeDtypeStruct((steps, split), F32),
        ],
        in_specs=[vmem] * 5,
        out_specs=[any_space, vmem],
        scratch_shapes=[
            pltpu.VMEM((chunks, rows_dev // chunks, split), F32),
            pltpu.SemaphoreType.DMA((chunks,)),
        ],
        compiler_params=pltpu.CompilerParams(vmem_limit_bytes=16 * 1024 * 1024),
        name="residual",
    )(held, pair, wide, kept, stat)
    return residual, norms


def solution(mesh):
    axes = tuple((name, mesh.shape[name]) for name in ("rows", "grp"))
    return jax.shard_map(
        functools.partial(on_device, axes),
        mesh=mesh,
        in_specs=(P(("rows", "grp"), None), P()),
        out_specs=(P(("rows", "grp"), None), P()),
        check_vma=False,
    )
```

```python
import functools

import jax
import jax.numpy as jnp
from jax import lax
from jax.experimental import pallas as pl
from jax.experimental.pallas import tpu as pltpu
from jax.sharding import PartitionSpec as P

PRIOR = 192
BLOCK = 8
HOOK_AT = 32
HIGH = lax.Precision.HIGHEST
LOGICAL = pl.DeviceIdType.LOGICAL
F32 = jnp.float32
BF16 = jnp.bfloat16


def dot(a, b, dims=((1,), (0,))):
    return lax.dot_general(a, b, (dims, ((), ())), precision=HIGH, preferred_element_type=F32)


def halves(value):
    hi = value.astype(BF16)
    return hi, (value - hi.astype(F32)).astype(BF16)


def flat_index(axes):
    (first, _), (second, width) = axes
    return lax.axis_index(first) * width + lax.axis_index(second)


def small_inverse(e):
    size = len(e)
    e = [list(line) for line in e]
    for p in range(size):
        inv = 1.0 / e[p][p]
        line = [e[p][j] * inv for j in range(size)]
        line[p] = -inv
        for i in range(size):
            for j in range(i, size):
                if i == p or j == p:
                    continue
                e[i][j] = e[i][j] - e[p][i] * line[j]
                e[j][i] = e[i][j]
        for j in range(size):
            e[p][j] = line[j]
            e[j][p] = line[j]
    return [[-value for value in line] for line in e]


def sweep_inverse(gram, hook, width=BLOCK):
    size = gram.shape[0]
    shape = (8, size)
    tiles = [gram[8 * t : 8 * t + 8, :] for t in range(size // 8)]
    lane = lax.broadcasted_iota(jnp.int32, shape, 1)
    sub = lax.broadcasted_iota(jnp.int32, shape, 0)
    for k in range(0, size, width):
        if k == HOOK_AT:
            hook()
        t, s = k // 8, k % 8
        inside = (lane >= k) & (lane < k + width)
        own = [jnp.broadcast_to(tiles[t][:, k + q : k + q + 1], shape) for q in range(width)]
        entry = [[None] * width for _ in range(width)]
        for p in range(width):
            for q in range(p, width):
                entry[p][q] = jnp.broadcast_to(own[q][s + p : s + p + 1, :], shape)
                entry[q][p] = entry[p][q]
        small = small_inverse(entry)
        rows = []
        for q in range(width):
            row = jnp.broadcast_to(tiles[t][s + q : s + q + 1, :], shape)
            rows.append(jnp.where(inside, jnp.where(lane == k + q, -1.0, 0.0), row))
        scaled = []
        for p in range(width):
            line = small[p][0] * rows[0]
            for q in range(1, width):
                line = line + small[p][q] * rows[q]
            scaled.append(line)
        fresh = []
        for r in range(size // 8):
            value = jnp.where(inside, 0.0, tiles[r])
            for p in range(width):
                col = own[p] if r == t else jnp.broadcast_to(tiles[r][:, k + p : k + p + 1], shape)
                value = value - col * scaled[p]
            fresh.append(value)
        for p in range(width):
            fresh[t] = jnp.where(sub == s + p, scaled[p], fresh[t])
        tiles = fresh
    return -jnp.concatenate(tiles, axis=0)


def reducers_of(n, tiles):
    count = min(tiles, n // 2)
    return count, n // 4, (n // 2) // count


def solve_kernel(
    axes, n, points_hbm, modes_ref, rest, pair, wide_ref, coef_ref, inverse_ref, stat_ref,
    points_ref, index_ref, fit, picked, acc, squares, part1, landed1, own1, full1, part2, landed2, own2, full2,
    listed, fit_in, rest_in, send1, recv1, share1, gather1, send2, recv2, share2, gather2,
):
    me = flat_index(axes)
    rows_dev, cols = modes_ref.shape
    split = cols // 2
    npts = points_ref.shape[0]
    padded = index_ref.shape[0]
    chunks = fit_in.shape[0]
    rows = rows_dev // chunks
    count, first, stride = reducers_of(n, split // 8)
    deep = split // count
    mine = (me - first) // stride
    reduces = (me >= first) & (me < first + count * stride) & (lax.rem(me - first + n, stride) == 0)

    def fetch_fit(c):
        at = pl.ds(c * rows, rows)
        return pltpu.make_async_copy(modes_ref.at[at, pl.ds(0, split)], fit.at[at, :], fit_in.at[c])

    def fetch_rest(c):
        at = pl.ds(c * rows, rows)
        return pltpu.make_async_copy(modes_ref.at[at, pl.ds(split, split)], rest.at[at, :], rest_in.at[c])

    def loop(body, start, stop, unroll=1):
        def step(i, carry):
            body(i)
            return carry

        lax.fori_loop(start, stop, step, 0, unroll=unroll)

    points_copy = pltpu.make_async_copy(points_hbm, points_ref, listed)
    points_copy.start()
    for c in range(chunks):
        fetch_fit(c).start()
    barrier = pltpu.get_barrier_semaphore()

    def greet(off):
        peer = lax.rem(me + off, n)
        pl.semaphore_signal(barrier, inc=1, device_id=peer, device_id_type=LOGICAL)

    loop(greet, 1, n)
    for c in range(chunks):
        fetch_rest(c).start()
    fit[rows_dev:, :] = jnp.zeros((8, split), F32)
    rest[rows_dev:, :] = jnp.zeros((8, split), F32)
    acc[...] = jnp.zeros_like(acc)
    squares[...] = jnp.zeros_like(squares)
    points_copy.wait()
    base = me * rows_dev

    def locate(i):
        at = points_ref[i] - base
        index_ref[i] = jnp.where((at >= 0) & (at < rows_dev), at, rows_dev)

    loop(locate, 0, npts, 4)
    for i in range(npts, padded):
        index_ref[i] = rows_dev

    def fit_gram(c):
        fetch_fit(c).wait()
        at = pl.ds(c * rows, rows)
        hi, lo = halves(fit[at, :])
        pair[at, :split] = hi
        pair[at, split:] = lo
        both = jnp.concatenate([hi, lo], axis=1)
        acc[:, :split] += lax.dot_general(both, hi, (((0,), (0,)), ((), ())), preferred_element_type=F32)

    def rest_gram(c):
        fetch_rest(c).wait()
        at = pl.ds(c * rows, rows)
        value = rest[at, :]
        hi, lo = halves(value)
        both = jnp.concatenate([hi, lo], axis=1)
        acc[:, split:] += lax.dot_general(pair[at, :], both, (((0,), (0,)), ((), ())), preferred_element_type=F32)
        squares[...] += jnp.sum((value * value).reshape(-1, 8, split), axis=0)

    def take(source, half):
        def pick(t):
            for s in range(8):
                picked[half, t, s : s + 1, :] = source[pl.ds(index_ref[t * 8 + s], 1), :]

        loop(pick, 0, padded // 8)

    def peer_copy(src, dst, sent, got, peer):
        return pltpu.make_async_remote_copy(
            src_ref=src, dst_ref=dst, send_sem=sent, recv_sem=got,
            device_id=peer, device_id_type=LOGICAL,
        )

    def scatter(part, landed, sent, got):
        def body(off):
            i = lax.rem(me + off, count)
            peer = first + i * stride

            @pl.when(peer != me)
            def _():
                peer_copy(part.at[i], landed.at[me], sent, got, peer).start()

        loop(body, 0, count)

    def reduce(part, landed, own, full, got, shared, gathered):
        @pl.when(reduces)
        def _():
            seen = landed.at[pl.ds(0, n - 1)]
            peer_copy(seen, seen, shared, got, me).wait_recv()
            landed[me] = part[mine]
            total = landed[0]
            for j in range(1, n):
                total = total + landed[j]
            own[...] = total
            full[mine] = total

            def body(off):
                peer = lax.rem(me + off, n)
                peer_copy(own, full.at[mine], shared, gathered, peer).start()

            loop(body, 1, n)

    def collect(full, shared, gathered):
        for held_here, size in ((reduces, count - 1), (jnp.logical_not(reduces), count)):

            @pl.when(held_here)
            def _():
                seen = full.at[pl.ds(0, size)]
                peer_copy(seen, seen, shared, gathered, me).wait_recv()

    def drain(part, landed, sent, shared):
        for held_here, size in ((reduces, count - 1), (jnp.logical_not(reduces), count)):

            @pl.when(held_here)
            def _():
                seen = part.at[pl.ds(0, size)]
                peer_copy(seen, seen, sent, shared, me).wait_send()

        @pl.when(reduces)
        def _():
            seen = landed.at[pl.ds(0, n - 1)]
            peer_copy(seen, seen, shared, sent, me).wait_send()

    with jax.named_scope("fgram"):
        loop(fit_gram, 0, chunks)
    with jax.named_scope("fpick"):
        take(fit, 0)
    with jax.named_scope("fdot"):
        left = picked[0].reshape(padded, split)
        part1[...] = dot(left, left, ((0,), (0,))).reshape(part1.shape)
    with jax.named_scope("barrier"):
        pl.semaphore_wait(barrier, n - 1)
    with jax.named_scope("scat1"):
        scatter(part1, landed1, send1, recv1)

    with jax.named_scope("rgram"):
        loop(rest_gram, 0, chunks)
    with jax.named_scope("rpick"):
        take(rest, 1)
    with jax.named_scope("rdot"):
        cross = dot(picked[0].reshape(padded, split), picked[1].reshape(padded, split), ((0,), (0,)))
        fold = acc[split:, :split]
        ftf = acc[:split, :split] + (fold + fold.T)
        ftr = acc[:split, split:cols] + (acc[:split, cols:] + acc[split:, split:cols])
        part2[...] = jnp.zeros_like(part2)
        part2[:, 0:deep, :] = cross.reshape(count, deep, split)
        part2[:, deep : 2 * deep, :] = ftf.reshape(count, deep, split)
        part2[:, 2 * deep : 3 * deep, :] = ftr.reshape(count, deep, split)
        fresh = npts - PRIOR - 1
        tail = slice(3 * deep, 3 * deep + 1)
        for i in range(fresh):
            for half in range(2):
                at = PRIOR + 1 + i
                part2[2 * i + half, tail, :] = picked[half, at // 8, at % 8 : at % 8 + 1, :]
        part2[2 * fresh, tail, :] = jnp.sum(squares[...], axis=0, keepdims=True)
    with jax.named_scope("scat2"):
        scatter(part2, landed2, send2, recv2)

    with jax.named_scope("red1"):
        reduce(part1, landed1, own1, full1, recv1, share1, gather1)
    with jax.named_scope("col1"):
        collect(full1, share1, gather1)

    def hook():
        with jax.named_scope("red2"):
            reduce(part2, landed2, own2, full2, recv2, share2, gather2)

    with jax.named_scope("sweep"):
        inverse = sweep_inverse(full1[...].reshape(split, split), hook)
    with jax.named_scope("col2"):
        collect(full2, share2, gather2)
    with jax.named_scope("coef"):
        coef = dot(inverse, full2[:, 0:deep, :].reshape(split, split))
        c_hi, c_lo = halves(coef)
        wide_ref[0:split, 0:split] = c_hi
        wide_ref[split:, 0:split] = c_hi
        wide_ref[0:split, split:] = c_lo
        wide_ref[split:, split:] = jnp.zeros((split, split), BF16)
        coef_ref[...] = coef
        inverse_ref[...] = inverse
        stat_ref[0:split, 0:split] = full2[:, deep : 2 * deep, :].reshape(split, split)
        stat_ref[0:split, split:] = full2[:, 2 * deep : 3 * deep, :].reshape(split, split)
        zero = jnp.zeros((8 - fresh, split), F32)
        for half in range(2):
            lines = [full2[2 * i + half, tail, :] for i in range(fresh)]
            stat_ref[split : split + 8, half * split : (half + 1) * split] = jnp.concatenate(lines + [zero], axis=0)
        stat_ref[split + 8 :, 0:split] = jnp.broadcast_to(full2[2 * fresh, tail, :], (8, split))
        stat_ref[split + 8 :, split:] = jnp.zeros((8, split), F32)
    with jax.named_scope("drain"):
        drain(part1, landed1, send1, share1)
        drain(part2, landed2, send2, share2)


def residual_kernel(
    total_rows, rest, pair, wide_ref, coef_ref, inverse_ref, stat_ref, res_ref, norm_ref, made_buf, norm_buf, wrote, normed
):
    chunks, rows, split = made_buf.shape
    steps = norm_buf.shape[0]
    fresh = steps - 1
    piece = 256 if rows % 256 == 0 else rows

    def flush(c):
        return pltpu.make_async_copy(made_buf.at[c], res_ref.at[pl.ds(c * rows, rows), :], wrote.at[c])

    wide = wide_ref[...]
    for c in range(chunks):
        for at in range(0, rows, piece):
            here = slice(c * rows + at, c * rows + at + piece)
            made = jnp.dot(pair[here, :], wide, preferred_element_type=F32)
            made_buf[c, at : at + piece, :] = rest[here, :] - (made[:, :split] + made[:, split:])
        flush(c).start()
    with jax.named_scope("chain"):
        coef = coef_ref[...]
        lefts = stat_ref[split : split + 8, 0:split]
        gains = dot(lefts, inverse_ref[...])
        errors = stat_ref[split : split + 8, split:] - dot(lefts, coef)
        kept = [coef]
        done = []
        pad7 = jnp.zeros((7, split), F32)
        for j in reversed(range(fresh)):
            left = lefts[j : j + 1, :]
            k = gains[j : j + 1, :]
            d = errors[j : j + 1, :]
            for k0, s0, d0 in done:
                along = jnp.sum(k0 * left, axis=1, keepdims=True)
                k = k + k0 * (along / s0)
                d = d + along * d0
            s = 1.0 - jnp.sum(k * left, axis=1, keepdims=True)
            d = d / s
            done.append((k, s, d))
            turn = dot(jnp.concatenate([k, pad7], axis=0), jnp.concatenate([d, pad7], axis=0), ((0,), (0,)))
            kept.append(kept[-1] - turn)
        kept = kept[::-1]
    with jax.named_scope("curved"):
        ftf, ftr = stat_ref[0:split, 0:split], stat_ref[0:split, split:]
        sq = stat_ref[split + 8 : split + 9, 0:split]
        curved = dot(ftf, jnp.concatenate(kept, axis=1))
        for j in range(steps):
            bent = kept[j] * (curved[:, j * split : (j + 1) * split] - 2.0 * ftr)
            norm_buf[j : j + 1, :] = (sq + jnp.sum(bent, axis=0, keepdims=True)) / total_rows
    norm_copy = pltpu.make_async_copy(norm_buf, norm_ref, normed)
    norm_copy.start()
    with jax.named_scope("flushwait"):
        for c in range(chunks):
            flush(c).wait()
        norm_copy.wait()


def on_device(axes, modes, points):
    n = axes[0][1] * axes[1][1]
    rows_dev, cols = modes.shape
    split = cols // 2
    npts = points.shape[0]
    steps = npts - PRIOR
    padded = -(-npts // 8) * 8
    count, _, _ = reducers_of(n, split // 8)
    deep = split // count
    vmem = pl.BlockSpec(memory_space=pltpu.VMEM)
    in_chunks = 6 if rows_dev % 96 == 0 else 1
    out_chunks = 12 if rows_dev % 96 == 0 else 1

    def buffers(depth):
        return [
            pltpu.VMEM((count, depth, split), F32),
            pltpu.VMEM((n, depth, split), F32),
            pltpu.VMEM((depth, split), F32),
            pltpu.VMEM((count, depth, split), F32),
        ]

    hbm = pl.BlockSpec(memory_space=pltpu.HBM)
    rest, pair, wide, coef, inverse, stat = pl.pallas_call(
        functools.partial(solve_kernel, axes, n),
        out_shape=[
            pltpu.VMEM((rows_dev + 8, split), F32),
            pltpu.VMEM((rows_dev, cols), BF16),
            pltpu.VMEM((cols, cols), BF16),
            pltpu.VMEM((split, split), F32),
            pltpu.VMEM((split, split), F32),
            pltpu.VMEM((split + 16, cols), F32),
        ],
        in_specs=[hbm] * 2,
        out_specs=[vmem] * 6,
        scratch_shapes=[
            pltpu.SMEM((npts,), jnp.int32),
            pltpu.SMEM((padded,), jnp.int32),
            pltpu.VMEM((rows_dev + 8, split), F32),
            pltpu.VMEM((2, padded // 8, 8, split), F32),
            pltpu.VMEM((cols, 3 * split), F32),
            pltpu.VMEM((8, split), F32),
        ]
        + buffers(deep)
        + buffers(3 * deep + 1)
        + [pltpu.SemaphoreType.DMA]
        + [pltpu.SemaphoreType.DMA((in_chunks,))] * 2
        + [pltpu.SemaphoreType.DMA] * 8,
        compiler_params=pltpu.CompilerParams(
            collective_id=0, has_side_effects=True, vmem_limit_bytes=24 * 1024 * 1024
        ),
        name="solve",
    )(pltpu.with_memory_space_constraint(points, pltpu.HBM), pltpu.with_memory_space_constraint(modes, pltpu.HBM))
    residual, norms = pl.pallas_call(
        functools.partial(residual_kernel, rows_dev * n),
        out_shape=[
            jax.ShapeDtypeStruct((rows_dev, split), F32),
            jax.ShapeDtypeStruct((steps, split), F32),
        ],
        in_specs=[vmem] * 6,
        out_specs=[hbm, hbm],
        scratch_shapes=[
            pltpu.VMEM((out_chunks, rows_dev // out_chunks, split), F32),
            pltpu.VMEM((steps, split), F32),
            pltpu.SemaphoreType.DMA((out_chunks,)),
            pltpu.SemaphoreType.DMA,
        ],
        compiler_params=pltpu.CompilerParams(vmem_limit_bytes=16 * 1024 * 1024),
        name="residual",
    )(rest, pair, wide, coef, inverse, stat)
    return residual, norms


def solution(mesh):
    axes = tuple((name, mesh.shape[name]) for name in ("rows", "grp"))
    return jax.shard_map(
        functools.partial(on_device, axes),
        mesh=mesh,
        in_specs=(P(("rows", "grp"), None), P()),
        out_specs=(P(("rows", "grp"), None), P()),
        check_vma=False,
    )
```

```python
import functools

import jax
import jax.numpy as jnp
from jax import lax
from jax.experimental import pallas as pl
from jax.experimental.pallas import tpu as pltpu
from jax.sharding import PartitionSpec as P

PRIOR = 192
BLOCK = 8
HOOK_FIT, HOOK_REST = 8, 24
WAVE = 1
HIGH = lax.Precision.HIGHEST
LOGICAL = pl.DeviceIdType.LOGICAL
F32 = jnp.float32
BF16 = jnp.bfloat16


def dot(a, b, dims=((1,), (0,))):
    return lax.dot_general(a, b, (dims, ((), ())), precision=HIGH, preferred_element_type=F32)


def halves(value):
    hi = value.astype(BF16)
    return hi, (value - hi.astype(F32)).astype(BF16)


def flat_index(axes):
    (first, _), (second, width) = axes
    return lax.axis_index(first) * width + lax.axis_index(second)


def small_inverse(e):
    size = len(e)
    e = [list(line) for line in e]
    for p in range(size):
        inv = 1.0 / e[p][p]
        line = [e[p][j] * inv for j in range(size)]
        line[p] = -inv
        for i in range(size):
            for j in range(i, size):
                if i == p or j == p:
                    continue
                e[i][j] = e[i][j] - e[p][i] * line[j]
                e[j][i] = e[i][j]
        for j in range(size):
            e[p][j] = line[j]
            e[j][p] = line[j]
    return [[-value for value in line] for line in e]


def sweep_inverse(gram, hook, width=BLOCK):
    size = gram.shape[0]
    shape = (8, size)
    tiles = [gram[8 * t : 8 * t + 8, :] for t in range(size // 8)]
    lane = lax.broadcasted_iota(jnp.int32, shape, 1)
    sub = lax.broadcasted_iota(jnp.int32, shape, 0)
    for k in range(0, size, width):
        hook(k)
        t, s = k // 8, k % 8
        inside = (lane >= k) & (lane < k + width)
        own = [jnp.broadcast_to(tiles[t][:, k + q : k + q + 1], shape) for q in range(width)]
        entry = [[None] * width for _ in range(width)]
        for p in range(width):
            for q in range(p, width):
                entry[p][q] = jnp.broadcast_to(own[q][s + p : s + p + 1, :], shape)
                entry[q][p] = entry[p][q]
        small = small_inverse(entry)
        rows = []
        for q in range(width):
            row = jnp.broadcast_to(tiles[t][s + q : s + q + 1, :], shape)
            rows.append(jnp.where(inside, jnp.where(lane == k + q, -1.0, 0.0), row))
        scaled = []
        for p in range(width):
            line = small[p][0] * rows[0]
            for q in range(1, width):
                line = line + small[p][q] * rows[q]
            scaled.append(line)
        fresh = []
        for r in range(size // 8):
            value = jnp.where(inside, 0.0, tiles[r])
            for p in range(width):
                col = own[p] if r == t else jnp.broadcast_to(tiles[r][:, k + p : k + p + 1], shape)
                value = value - col * scaled[p]
            fresh.append(value)
        for p in range(width):
            fresh[t] = jnp.where(sub == s + p, scaled[p], fresh[t])
        tiles = fresh
    return -jnp.concatenate(tiles, axis=0)


def reducers_of(n, tiles):
    count = min(tiles // 2, n // 4)
    return count, n // 4 + 1, (n // 2) // count


def solve_kernel(
    axes, n, points_hbm, modes_ref, rest, pair, wide_ref, coef_ref, inverse_ref, stat_ref,
    points_ref, index_ref, fit, turned, picked, acc1, acc2, squares,
    part1, landed1, own1, full1, part2, landed2, own2, full2, part3, landed3, own3, full3,
    listed, fit_in, rest_in, send1, recv1, share1, gather1, send2, recv2, share2, gather2, send3, recv3, share3, gather3,
):
    me = flat_index(axes)
    rows_dev, cols = modes_ref.shape
    split = cols // 2
    npts = points_ref.shape[0]
    padded = index_ref.shape[0]
    chunks = fit_in.shape[0]
    rows = rows_dev // chunks
    count, first, stride = reducers_of(n, split // 8)
    deep = split // count
    mine = (me - first) // stride
    reduces = (me >= first) & (me < first + count * stride) & (lax.rem(me - first + n, stride) == 0)

    def fetch_fit(c):
        at = pl.ds(c * rows, rows)
        return pltpu.make_async_copy(modes_ref.at[at, pl.ds(0, split)], fit.at[at, :], fit_in.at[c])

    def fetch_rest(c):
        at = pl.ds(c * rows, rows)
        return pltpu.make_async_copy(modes_ref.at[at, pl.ds(split, split)], rest.at[at, :], rest_in.at[c])

    def loop(body, start, stop, unroll=1):
        def step(i, carry):
            body(i)
            return carry

        lax.fori_loop(start, stop, step, 0, unroll=unroll)

    points_copy = pltpu.make_async_copy(points_hbm, points_ref, listed)
    points_copy.start()
    for c in range(chunks):
        fetch_fit(c).start()
    barrier = pltpu.get_barrier_semaphore()

    def greet(off):
        peer = lax.rem(me + off, n)
        pl.semaphore_signal(barrier, inc=1, device_id=peer, device_id_type=LOGICAL)

    loop(greet, 1, n)
    for c in range(chunks):
        fetch_rest(c).start()
    fit[rows_dev:, :] = jnp.zeros((8, split), F32)
    rest[rows_dev:, :] = jnp.zeros((8, split), F32)
    for total in (acc1, acc2, squares):
        total[...] = jnp.zeros_like(total)
    points_copy.wait()
    base = me * rows_dev

    def locate(i):
        at = points_ref[i] - base
        index_ref[i] = jnp.where((at >= 0) & (at < rows_dev), at, rows_dev)

    loop(locate, 0, npts, 4)
    for i in range(npts, padded):
        index_ref[i] = rows_dev

    wave = WAVE if chunks % WAVE == 0 else 1
    plain = (((1,), (0,)), ((), ()))

    def pieces_of(c):
        size = wave * rows // 2
        return [(i, slice(c * wave * rows + i * size, c * wave * rows + (i + 1) * size)) for i in range(2)]

    def fit_gram(c):
        for i, at in pieces_of(c):
            hi, lo = halves(fit[at, :])
            pair[at, :split] = hi
            pair[at, split:] = lo
            flip = hi.T
            turned[:, at] = flip
            acc1[i] += lax.dot_general(flip, jnp.concatenate([hi, lo], axis=1), plain, preferred_element_type=F32)

    def rest_gram(c):
        for i in range(wave):
            fetch_rest(c * wave + i).wait()
        for i, at in pieces_of(c):
            value = rest[at, :]
            hi, lo = halves(value)
            both = jnp.concatenate([turned[:, at], pair[at, split:].T], axis=0)
            acc2[i] += lax.dot_general(both, jnp.concatenate([hi, lo], axis=1), plain, preferred_element_type=F32)
            squares[...] += jnp.sum((value * value).reshape(-1, 8, split), axis=0)

    def take(source, half):
        def pick(t):
            for s in range(8):
                picked[half, t, s : s + 1, :] = source[pl.ds(index_ref[t * 8 + s], 1), :]

        loop(pick, 0, padded // 8)

    def peer_copy(src, dst, sent, got, peer):
        return pltpu.make_async_remote_copy(
            src_ref=src, dst_ref=dst, send_sem=sent, recv_sem=got,
            device_id=peer, device_id_type=LOGICAL,
        )

    def scatter(part, landed, sent, got):
        def body(off):
            i = lax.rem(me + off, count)
            peer = first + i * stride

            @pl.when(peer != me)
            def _():
                peer_copy(part.at[i], landed.at[me], sent, got, peer).start()

        loop(body, 0, count)

    def reduce(pieces, own, full, shared, gathered):
        @pl.when(reduces)
        def _():
            at = 0
            for part, landed, got in pieces:
                seen = landed.at[pl.ds(0, n - 1)]
                peer_copy(seen, seen, shared, got, me).wait_recv()
                landed[me] = part[mine]
                total = landed[0]
                for j in range(1, n):
                    total = total + landed[j]
                own[at : at + total.shape[0], :] = total
                at += total.shape[0]
            full[mine] = own[...]

            def body(off):
                peer = lax.rem(me + off, n)
                peer_copy(own, full.at[mine], shared, gathered, peer).start()

            loop(body, 1, n)

    def collect(full, shared, gathered):
        for held_here, size in ((reduces, count - 1), (jnp.logical_not(reduces), count)):

            @pl.when(held_here)
            def _():
                seen = full.at[pl.ds(0, size)]
                peer_copy(seen, seen, shared, gathered, me).wait_recv()

    def drain(parts, full, shared):
        for held_here, size in ((reduces, count - 1), (jnp.logical_not(reduces), count)):

            @pl.when(held_here)
            def _():
                for part, sent in parts:
                    seen = part.at[pl.ds(0, size)]
                    peer_copy(seen, seen, sent, shared, me).wait_send()

        @pl.when(reduces)
        def _():
            seen = full.at[pl.ds(0, count)]
            for _ in range((n - 1) // count):
                peer_copy(seen, seen, shared, shared, me).wait_send()
            rest_of = full.at[pl.ds(0, (n - 1) % count)]
            peer_copy(rest_of, rest_of, shared, shared, me).wait_send()

    waves = chunks // wave
    with jax.named_scope("fgram"):
        for c in range(waves):
            for i in range(wave):
                fetch_fit(c * wave + i).wait()
            if c < waves - 1:
                fit_gram(c)
    with jax.named_scope("fpick"):
        take(fit, 0)
    with jax.named_scope("fdot"):
        left = picked[0].reshape(padded, split)
        part1[...] = dot(left, left, ((0,), (0,))).reshape(part1.shape)
    with jax.named_scope("barrier"):
        pl.semaphore_wait(barrier, n - 1)
    with jax.named_scope("scat1"):
        scatter(part1, landed1, send1, recv1)

    with jax.named_scope("fgram2"):
        fit_gram(waves - 1)
    for c in range(waves):
        with jax.named_scope("rgram"):
            rest_gram(c)
        if c == 0:
            with jax.named_scope("scat2"):
                total = acc1[0] + acc1[1]
                cross = total[:, split:]
                part2[...] = (total[:, :split] + (cross + cross.T)).reshape(part2.shape)
                scatter(part2, landed2, send2, recv2)
    with jax.named_scope("rpick"):
        take(rest, 1)
    with jax.named_scope("rdot"):
        cross = dot(picked[0].reshape(padded, split), picked[1].reshape(padded, split), ((0,), (0,)))
        total = acc2[0] + acc2[1]
        ftr = total[:split, :split] + (total[:split, split:] + total[split:, :split])
        fresh = npts - PRIOR - 1
        tail = slice(2 * deep, 2 * deep + 1)
        part3[:, tail, :] = jnp.zeros((count, 1, split), F32)
        part3[:, 0:deep, :] = cross.reshape(count, deep, split)
        part3[:, deep : 2 * deep, :] = ftr.reshape(count, deep, split)
        for i in range(fresh):
            for half in range(2):
                at = PRIOR + 1 + i
                part3[2 * i + half, tail, :] = picked[half, at // 8, at % 8 : at % 8 + 1, :]
        part3[2 * fresh, tail, :] = jnp.sum(squares[...], axis=0, keepdims=True)
    with jax.named_scope("scat3"):
        scatter(part3, landed3, send3, recv3)

    with jax.named_scope("red1"):
        reduce([(part1, landed1, recv1)], own1, full1, share1, gather1)
    with jax.named_scope("col1"):
        collect(full1, share1, gather1)

    def hook(k):
        if k == HOOK_FIT:
            with jax.named_scope("red2"):
                reduce([(part2, landed2, recv2)], own2, full2, share2, gather2)
        if k == HOOK_REST:
            with jax.named_scope("red3"):
                reduce([(part3, landed3, recv3)], own3, full3, share3, gather3)

    with jax.named_scope("sweep"):
        inverse = sweep_inverse(full1[...].reshape(split, split), hook)
    with jax.named_scope("col3"):
        collect(full3, share3, gather3)
    with jax.named_scope("coef"):
        coef = dot(inverse, full3[:, 0:deep, :].reshape(split, split))
        c_hi, c_lo = halves(coef)
        wide_ref[0:split, 0:split] = c_hi
        wide_ref[split:, 0:split] = c_hi
        wide_ref[0:split, split:] = c_lo
        wide_ref[split:, split:] = jnp.zeros((split, split), BF16)
        coef_ref[...] = coef
        inverse_ref[...] = inverse
        stat_ref[0:split, split:] = full3[:, deep : 2 * deep, :].reshape(split, split)
        zero = jnp.zeros((8 - fresh, split), F32)
        for half in range(2):
            lines = [full3[2 * i + half, tail, :] for i in range(fresh)]
            stat_ref[split : split + 8, half * split : (half + 1) * split] = jnp.concatenate(lines + [zero], axis=0)
        stat_ref[split + 8 :, 0:split] = jnp.broadcast_to(full3[2 * fresh, tail, :], (8, split))
        stat_ref[split + 8 :, split:] = jnp.zeros((8, split), F32)
    with jax.named_scope("col2"):
        collect(full2, share2, gather2)
        stat_ref[0:split, 0:split] = full2[...].reshape(split, split)
    with jax.named_scope("drain"):
        drain([(part1, send1)], full1, share1)
        drain([(part2, send2)], full2, share2)
        drain([(part3, send3)], full3, share3)


def residual_kernel(
    total_rows, rest, pair, wide_ref, coef_ref, inverse_ref, stat_ref, res_ref, norm_ref, made_buf, norm_buf, wrote, normed
):
    chunks, rows, split = made_buf.shape
    steps = norm_buf.shape[0]
    fresh = steps - 1
    piece = 256 if rows % 256 == 0 else rows

    def flush(c):
        return pltpu.make_async_copy(made_buf.at[c], res_ref.at[pl.ds(c * rows, rows), :], wrote.at[c])

    wide = wide_ref[...]
    for c in range(chunks):
        for at in range(0, rows, piece):
            here = slice(c * rows + at, c * rows + at + piece)
            made = jnp.dot(pair[here, :], wide, preferred_element_type=F32)
            made_buf[c, at : at + piece, :] = rest[here, :] - (made[:, :split] + made[:, split:])
        flush(c).start()
    with jax.named_scope("chain"):
        coef = coef_ref[...]
        lefts = stat_ref[split : split + 8, 0:split]
        gains = dot(lefts, inverse_ref[...])
        errors = stat_ref[split : split + 8, split:] - dot(lefts, coef)
        kept = [coef]
        done = []
        pad7 = jnp.zeros((7, split), F32)
        for j in reversed(range(fresh)):
            left = lefts[j : j + 1, :]
            k = gains[j : j + 1, :]
            d = errors[j : j + 1, :]
            for k0, s0, d0 in done:
                along = jnp.sum(k0 * left, axis=1, keepdims=True)
                k = k + k0 * (along / s0)
                d = d + along * d0
            s = 1.0 - jnp.sum(k * left, axis=1, keepdims=True)
            d = d / s
            done.append((k, s, d))
            turn = dot(jnp.concatenate([k, pad7], axis=0), jnp.concatenate([d, pad7], axis=0), ((0,), (0,)))
            kept.append(kept[-1] - turn)
        kept = kept[::-1]
    with jax.named_scope("curved"):
        ftf, ftr = stat_ref[0:split, 0:split], stat_ref[0:split, split:]
        sq = stat_ref[split + 8 : split + 9, 0:split]
        curved = dot(ftf, jnp.concatenate(kept, axis=1))
        for j in range(steps):
            bent = kept[j] * (curved[:, j * split : (j + 1) * split] - 2.0 * ftr)
            norm_buf[j : j + 1, :] = (sq + jnp.sum(bent, axis=0, keepdims=True)) / total_rows
    norm_copy = pltpu.make_async_copy(norm_buf, norm_ref, normed)
    norm_copy.start()
    with jax.named_scope("flushwait"):
        for c in range(chunks):
            flush(c).wait()
        norm_copy.wait()


def on_device(axes, modes, points):
    n = axes[0][1] * axes[1][1]
    rows_dev, cols = modes.shape
    split = cols // 2
    npts = points.shape[0]
    steps = npts - PRIOR
    padded = -(-npts // 8) * 8
    count, _, _ = reducers_of(n, split // 8)
    deep = split // count
    vmem = pl.BlockSpec(memory_space=pltpu.VMEM)
    in_chunks = 6 if rows_dev % 96 == 0 else 1
    out_chunks = 12 if rows_dev % 96 == 0 else 1

    def sources(depth):
        return [pltpu.VMEM((count, depth, split), F32), pltpu.VMEM((n, depth, split), F32)]

    def sums(depth):
        return [pltpu.VMEM((depth, split), F32), pltpu.VMEM((count, depth, split), F32)]

    hbm = pl.BlockSpec(memory_space=pltpu.HBM)
    rest, pair, wide, coef, inverse, stat = pl.pallas_call(
        functools.partial(solve_kernel, axes, n),
        out_shape=[
            pltpu.VMEM((rows_dev + 8, split), F32),
            pltpu.VMEM((rows_dev, cols), BF16),
            pltpu.VMEM((cols, cols), BF16),
            pltpu.VMEM((split, split), F32),
            pltpu.VMEM((split, split), F32),
            pltpu.VMEM((split + 16, cols), F32),
        ],
        in_specs=[hbm] * 2,
        out_specs=[vmem] * 6,
        scratch_shapes=[
            pltpu.SMEM((npts,), jnp.int32),
            pltpu.SMEM((padded,), jnp.int32),
            pltpu.VMEM((rows_dev + 8, split), F32),
            pltpu.VMEM((split, rows_dev), BF16),
            pltpu.VMEM((2, padded // 8, 8, split), F32),
            pltpu.VMEM((2, split, cols), F32),
            pltpu.VMEM((2, cols, cols), F32),
            pltpu.VMEM((8, split), F32),
        ]
        + sources(deep)
        + sums(deep)
        + sources(deep)
        + sums(deep)
        + sources(2 * deep + 1)
        + sums(2 * deep + 1)
        + [pltpu.SemaphoreType.DMA]
        + [pltpu.SemaphoreType.DMA((in_chunks,))] * 2
        + [pltpu.SemaphoreType.DMA] * 12,
        compiler_params=pltpu.CompilerParams(
            collective_id=0, has_side_effects=True, vmem_limit_bytes=24 * 1024 * 1024
        ),
        name="solve",
    )(pltpu.with_memory_space_constraint(points, pltpu.HBM), pltpu.with_memory_space_constraint(modes, pltpu.HBM))
    residual, norms = pl.pallas_call(
        functools.partial(residual_kernel, rows_dev * n),
        out_shape=[
            jax.ShapeDtypeStruct((rows_dev, split), F32),
            jax.ShapeDtypeStruct((steps, split), F32),
        ],
        in_specs=[vmem] * 6,
        out_specs=[hbm, hbm],
        scratch_shapes=[
            pltpu.VMEM((out_chunks, rows_dev // out_chunks, split), F32),
            pltpu.VMEM((steps, split), F32),
            pltpu.SemaphoreType.DMA((out_chunks,)),
            pltpu.SemaphoreType.DMA,
        ],
        compiler_params=pltpu.CompilerParams(vmem_limit_bytes=16 * 1024 * 1024),
        name="residual",
    )(rest, pair, wide, coef, inverse, stat)
    return residual, norms


def solution(mesh):
    axes = tuple((name, mesh.shape[name]) for name in ("rows", "grp"))
    return jax.shard_map(
        functools.partial(on_device, axes),
        mesh=mesh,
        in_specs=(P(("rows", "grp"), None), P()),
        out_specs=(P(("rows", "grp"), None), P()),
        check_vma=False,
    )
```

```python
import functools

import jax
import jax.numpy as jnp
from jax import lax
from jax.experimental import pallas as pl
from jax.experimental.pallas import tpu as pltpu
from jax.sharding import PartitionSpec as P

PRIOR = 192
HOOK_REST, HOOK_FIT = 8, 24
WAVE = 1
UNROLL = 8
SEND_FIT = 3
HIGH = lax.Precision.HIGHEST
LOGICAL = pl.DeviceIdType.LOGICAL
F32 = jnp.float32
BF16 = jnp.bfloat16


def dot(a, b, dims=((1,), (0,))):
    return lax.dot_general(a, b, (dims, ((), ())), precision=HIGH, preferred_element_type=F32)


def halves(value):
    hi = value.astype(BF16)
    return hi, (value - hi.astype(F32)).astype(BF16)


def flat_index(axes):
    (first, _), (second, width) = axes
    return lax.axis_index(first) * width + lax.axis_index(second)


def small_inverse(e):
    size = len(e)
    e = [list(line) for line in e]
    for p in range(size):
        inv = 1.0 / e[p][p]
        line = [e[p][j] * inv for j in range(size)]
        line[p] = -inv
        for i in range(size):
            for j in range(i, size):
                if i == p or j == p:
                    continue
                e[i][j] = e[i][j] - e[p][i] * line[j]
                e[j][i] = e[i][j]
        for j in range(size):
            e[p][j] = line[j]
            e[j][p] = line[j]
    return [[-value for value in line] for line in e]


def added(terms):
    while len(terms) > 1:
        pairs = [terms[i] + terms[i + 1] for i in range(0, len(terms) - 1, 2)]
        terms = pairs + terms[len(pairs) * 2 :]
    return terms[0]


def sweep_inverse(gram, hook, line_ref, column_ref):
    size = gram.shape[0]
    steps = size // 8
    shape = (8, size)
    wide = (8, line_ref.shape[-1])
    tiles = [gram[8 * t : 8 * t + 8, :] for t in range(steps)]
    lane = lax.broadcasted_iota(jnp.int32, shape, 1)
    sub = lax.broadcasted_iota(jnp.int32, shape, 0)

    def column(tile, at):
        return jnp.broadcast_to(tile[:, at : at + 1], shape)

    for t in range(steps):
        k = 8 * t
        hook(k)
        own = [column(tiles[t], k + q) for q in range(8)]
        line_ref[t, :, 0:size] = tiles[t]
        for q in range(8):
            column_ref[t, q, :, 0:size] = own[q]
        entry = [[None] * 8 for _ in range(8)]
        for p in range(8):
            for q in range(p, 8):
                entry[p][q] = jnp.broadcast_to(column_ref[t, q, p : p + 1, 0:size], shape)
                entry[q][p] = entry[p][q]
        small = small_inverse(entry)
        inside = (lane >= k) & (lane < k + 8)
        rows = []
        for q in range(8):
            row = jnp.broadcast_to(line_ref[t, q : q + 1, 0:size], shape)
            rows.append(jnp.where(inside, jnp.where(lane == k + q, -1.0, 0.0), row))
        scaled = [added([small[p][q] * rows[q] for q in range(8)]) for p in range(8)]
        fresh = []
        for r in range(steps):
            columns = own if r == t else [column(tiles[r], k + p) for p in range(8)]
            value = jnp.where(inside, 0.0, tiles[r])
            fresh.append(value - added([columns[p] * scaled[p] for p in range(8)]))
        for p in range(8):
            fresh[t] = jnp.where(sub == p, scaled[p], fresh[t])
        tiles = fresh
    return -jnp.concatenate(tiles, axis=0)


def reducers_of(n, tiles):
    count = min(tiles // 2, n // 4)
    return count, n // 4 + 1, (n // 2) // count


def solve_kernel(
    axes, n, points_hbm, modes_ref, rest, pair, wide_ref, coef_ref, inverse_ref, stat_ref,
    points_ref, index_ref, fit, turned, picked, acc1, acc2, squares,
    part1, landed1, own1, full1, part2, mate2, landed2, own2, full2, part3, mate3, landed3, part4, mate4, landed4, own3, full3, line_ref, column_ref,
    listed, fit_in, rest_in, sems,
):
    me = flat_index(axes)
    rows_dev, cols = modes_ref.shape
    split = cols // 2
    npts = points_ref.shape[0]
    padded = index_ref.shape[0]
    chunks = fit_in.shape[0]
    rows = rows_dev // chunks
    count, first, stride = reducers_of(n, split // 8)
    deep = split // count
    mine = (me - first) // stride
    pairs = n // 2
    side = lax.rem(me, 2)
    partner = me + 1 - 2 * side
    (send1, recv1, share1, gather1, send2, recv2, share2, gather2, send3, recv3, send4, recv4, share3, gather3) = [
        sems.at[i] for i in range(14)
    ]
    swaps = [(sems.at[14 + 2 * i], sems.at[15 + 2 * i]) for i in range(3)]
    reduces = (me >= first) & (me < first + count * stride) & (lax.rem(me - first + n, stride) == 0)

    def fetch_fit(c):
        at = pl.ds(c * rows, rows)
        return pltpu.make_async_copy(modes_ref.at[at, pl.ds(0, split)], fit.at[at, :], fit_in.at[c])

    def fetch_rest(c):
        at = pl.ds(c * rows, rows)
        return pltpu.make_async_copy(modes_ref.at[at, pl.ds(split, split)], rest.at[at, :], rest_in.at[c])

    def loop(body, start, stop, unroll=1):
        def step(i, carry):
            body(i)
            return carry

        lax.fori_loop(start, stop, step, 0, unroll=unroll)

    points_copy = pltpu.make_async_copy(points_hbm, points_ref, listed)
    points_copy.start()
    for c in range(chunks):
        fetch_fit(c).start()
    barrier = pltpu.get_barrier_semaphore()

    def greet(off):
        peer = lax.rem(me + off, n)
        pl.semaphore_signal(barrier, inc=1, device_id=peer, device_id_type=LOGICAL)

    loop(greet, 1, n)
    fit[rows_dev:, :] = jnp.zeros((8, split), F32)
    rest[rows_dev:, :] = jnp.zeros((8, split), F32)
    for total in (acc1, acc2, squares):
        total[...] = jnp.zeros_like(total)
    points_copy.wait()
    base = me * rows_dev

    def locate(i):
        at = points_ref[i] - base
        index_ref[i] = jnp.where((at >= 0) & (at < rows_dev), at, rows_dev)

    loop(locate, 0, npts, 4)
    for i in range(npts, padded):
        index_ref[i] = rows_dev

    wave = WAVE if chunks % WAVE == 0 else 1
    plain = (((1,), (0,)), ((), ()))

    def pieces_of(c):
        size = wave * rows // 2
        return [(i, slice(c * wave * rows + i * size, c * wave * rows + (i + 1) * size)) for i in range(2)]

    def fit_gram(c):
        for i, at in pieces_of(c):
            hi, lo = halves(fit[at, :])
            pair[at, :split] = hi
            pair[at, split:] = lo
            flip = hi.T
            turned[:, at] = flip
            acc1[i] += lax.dot_general(flip, jnp.concatenate([hi, lo], axis=1), plain, preferred_element_type=F32)

    def rest_gram(c):
        for i in range(wave):
            fetch_rest(c * wave + i).wait()
        for i, at in pieces_of(c):
            value = rest[at, :]
            hi, lo = halves(value)
            both = jnp.concatenate([turned[:, at], pair[at, split:].T], axis=0)
            acc2[i] += lax.dot_general(both, jnp.concatenate([hi, lo], axis=1), plain, preferred_element_type=F32)
            squares[...] += jnp.sum((value * value).reshape(-1, 8, split), axis=0)

    def take(source, half):
        def pick(t):
            for s in range(8):
                picked[half, t, s : s + 1, :] = source[pl.ds(index_ref[t * 8 + s], 1), :]

        loop(pick, 0, padded // 8)

    def peer_copy(src, dst, sent, got, peer):
        return pltpu.make_async_remote_copy(
            src_ref=src, dst_ref=dst, send_sem=sent, recv_sem=got,
            device_id=peer, device_id_type=LOGICAL,
        )

    def scatter(part, landed, sent, got):
        def body(off):
            i = lax.rem(me + 3 * off, count)
            peer = first + i * stride

            @pl.when(peer != me)
            def _():
                peer_copy(part.at[i], landed.at[me], sent, got, peer).start()

        loop(body, 0, count, UNROLL)

    def fill(part, value):
        for i in range(count):
            part[i % 2, i // 2, 0:deep, :] = value[i * deep : (i + 1) * deep, :]

    def swap(part, mate, sems_of):
        return peer_copy(part.at[1 - side], mate, *sems_of, partner)

    def scatter_pair(part, mate, landed, sems_of, sent, got):
        swap(part, mate, sems_of).wait_recv()
        part[side] = part[side] + mate[...]

        def body(off):
            i = lax.rem(me // 2 + off, count // 2)
            peer = first + (2 * i + side) * stride

            @pl.when(peer != me)
            def _():
                peer_copy(part.at[side, i], landed.at[me // 2], sent, got, peer).start()

        loop(body, 0, count // 2, UNROLL)

    local_pair = reduces & (lax.rem(mine + 2 * n, 2) == side)
    other_pair = reduces & (lax.rem(mine + 2 * n, 2) != side)

    def share(own, full, shared, gathered):
        full[mine] = own[...]

        def body(off):
            ahead = off + n // 4 - 1
            peer = lax.rem(me + jnp.where(ahead < n, ahead, ahead - n + 1), n)
            peer_copy(own, full.at[mine], shared, gathered, peer).start()

        loop(body, 1, n, UNROLL)

    def summed(landed):
        return added([landed[j] for j in range(landed.shape[0])])

    def reduce_all(part, landed, own, full, got, shared, gathered):
        @pl.when(reduces)
        def _():
            seen = landed.at[pl.ds(0, n - 1)]
            peer_copy(seen, seen, shared, got, me).wait_recv()
            landed[me] = part[mine]
            own[...] = summed(landed)
            share(own, full, shared, gathered)

    def reduce_pairs(pieces, own, full, shared, gathered):
        @pl.when(local_pair)
        def _():
            for part, landed, got in pieces:
                seen = landed.at[pl.ds(0, pairs - 1)]
                peer_copy(seen, seen, shared, got, me).wait_recv()
                landed[me // 2] = part[side, mine // 2]

        @pl.when(other_pair)
        def _():
            for part, landed, got in pieces:
                seen = landed.at[pl.ds(0, pairs)]
                peer_copy(seen, seen, shared, got, me).wait_recv()

        @pl.when(reduces)
        def _():
            at = 0
            for part, landed, got in pieces:
                own[at : at + landed.shape[1], :] = summed(landed)
                at += landed.shape[1]
            share(own, full, shared, gathered)

    def collect(full, shared, gathered):
        for held_here, size in ((reduces, count - 1), (jnp.logical_not(reduces), count)):

            @pl.when(held_here)
            def _():
                seen = full.at[pl.ds(0, size)]
                peer_copy(seen, seen, shared, gathered, me).wait_recv()

    def drain_shared(full, shared):
        @pl.when(reduces)
        def _():
            seen = full.at[pl.ds(0, count)]
            for _ in range((n - 1) // count):
                peer_copy(seen, seen, shared, shared, me).wait_send()
            rest_of = full.at[pl.ds(0, (n - 1) % count)]
            peer_copy(rest_of, rest_of, shared, shared, me).wait_send()

    def drain_sent(pieces, skips, size):
        for held_here, some in ((skips, size - 1), (jnp.logical_not(skips), size)):

            @pl.when(held_here)
            def _():
                for part, sent in pieces:
                    seen = part.at[pl.ds(0, some)]
                    peer_copy(seen, seen, sent, sent, me).wait_send()

    waves = chunks // wave
    with jax.named_scope("fgram"):
        for c in range(waves):
            for i in range(wave):
                fetch_fit(c * wave + i).wait()
            if c == max(waves - 3, 0):
                for i in range(chunks):
                    fetch_rest(i).start()
            if c < waves - 1:
                fit_gram(c)
    with jax.named_scope("fpick"):
        take(fit, 0)
    with jax.named_scope("fdot"):
        left = picked[0].reshape(padded, split)
        part1[...] = dot(left, left, ((0,), (0,))).reshape(part1.shape)
    with jax.named_scope("barrier"):
        pl.semaphore_wait(barrier, n - 1)
    with jax.named_scope("scat1"):
        scatter(part1, landed1, send1, recv1)

    with jax.named_scope("fgram2"):
        fit_gram(waves - 1)
        total = acc1[0] + acc1[1]
        cross = total[:, split:]
        fill(part2, total[:, :split] + (cross + cross.T))
        swap(part2, mate2, swaps[0]).start()
    for c in range(waves):
        with jax.named_scope("rgram"):
            rest_gram(c)
        if c == SEND_FIT:
            with jax.named_scope("scat2"):
                scatter_pair(part2, mate2, landed2, swaps[0], send2, recv2)
    with jax.named_scope("swap3"):
        total = acc2[0] + acc2[1]
        fill(part3, total[:split, :split] + (total[:split, split:] + total[split:, :split]))
        swap(part3, mate3, swaps[1]).start()
    with jax.named_scope("rpick"):
        take(rest, 1)
    with jax.named_scope("rdot"):
        fresh = npts - PRIOR - 1
        tail = slice(deep, deep + 1)
        part4[:, :, tail, :] = jnp.zeros((2, count // 2, 1, split), F32)
        fill(part4, dot(picked[0].reshape(padded, split), picked[1].reshape(padded, split), ((0,), (0,))))
        for i in range(fresh):
            for side_of in range(2):
                at = PRIOR + 1 + i
                part4[side_of, i, tail, :] = picked[side_of, at // 8, at % 8 : at % 8 + 1, :]
        part4[0, fresh, tail, :] = jnp.sum(squares[...], axis=0, keepdims=True)
        swap(part4, mate4, swaps[2]).start()
    with jax.named_scope("scat3"):
        scatter_pair(part3, mate3, landed3, swaps[1], send3, recv3)
    with jax.named_scope("scat4"):
        scatter_pair(part4, mate4, landed4, swaps[2], send4, recv4)

    with jax.named_scope("red1"):
        reduce_all(part1, landed1, own1, full1, recv1, share1, gather1)
    with jax.named_scope("col1"):
        collect(full1, share1, gather1)

    half = split // 2

    def hook(k):
        if k == HOOK_REST:
            with jax.named_scope("red3"):
                reduce_pairs([(part4, landed4, recv4)], own3, full3, share3, gather3)
        if k == HOOK_FIT:
            with jax.named_scope("red2"):
                reduce_pairs([(part2, landed2, recv2), (part3, landed3, recv3)], own2, full2, share2, gather2)

    with jax.named_scope("sweepP"):
        gram = full1[...].reshape(split, split)
        upper = sweep_inverse(gram[:half, :half], hook, line_ref, column_ref)
    with jax.named_scope("mid"):
        corner = gram[:half, half:]
        link = dot(upper, corner)
        schur = gram[half:, half:] - dot(corner, link, ((0,), (0,)))
    with jax.named_scope("sweepZ"):
        later = pl.ds(half // 8, half // 8)
        lower = sweep_inverse(schur, lambda k: None, line_ref.at[later], column_ref.at[later])
    with jax.named_scope("join"):
        bridge = dot(link, lower)
        above = jnp.concatenate([upper + dot(bridge, link, ((1,), (1,))), -bridge], axis=1)
        inverse = jnp.concatenate([above, jnp.concatenate([-bridge.T, lower], axis=1)], axis=0)
        inverse_ref[...] = inverse
    with jax.named_scope("col3"):
        collect(full3, share3, gather3)
    with jax.named_scope("coef"):
        coef = dot(inverse, full3[:, 0:deep, :].reshape(split, split))
        c_hi, c_lo = halves(coef)
        wide_ref[0:split, 0:split] = c_hi
        wide_ref[split:, 0:split] = c_hi
        wide_ref[0:split, split:] = c_lo
        wide_ref[split:, split:] = jnp.zeros((split, split), BF16)
        coef_ref[...] = coef
        zero = jnp.zeros((8 - fresh, split), F32)
        for part in range(2):
            lines = [full3[2 * i + part, tail, :] for i in range(fresh)]
            stat_ref[split : split + 8, part * split : (part + 1) * split] = jnp.concatenate(lines + [zero], axis=0)
        stat_ref[split + 8 :, 0:split] = jnp.broadcast_to(full3[2 * fresh, tail, :], (8, split))
        stat_ref[split + 8 :, split:] = jnp.zeros((8, split), F32)
    with jax.named_scope("col2"):
        collect(full2, share2, gather2)
        stat_ref[0:split, 0:split] = full2[:, 0:deep, :].reshape(split, split)
        stat_ref[0:split, split:] = full2[:, deep:, :].reshape(split, split)
    with jax.named_scope("drain"):
        drain_sent([(part1, send1)], reduces, count)
        drain_sent([(mate2, send2), (mate3, send3), (mate4, send4)], local_pair, count // 2)
        for part, mate, sems_of in ((part2, mate2, swaps[0]), (part3, mate3, swaps[1]), (part4, mate4, swaps[2])):
            swap(part, mate, sems_of).wait_send()
        for full, shared in ((full1, share1), (full2, share2), (full3, share3)):
            drain_shared(full, shared)


def residual_kernel(
    total_rows, rest, pair, wide_ref, coef_ref, inverse_ref, stat_ref, res_ref, norm_ref, made_buf, norm_buf, wrote, normed
):
    chunks, rows, split = made_buf.shape
    steps = norm_buf.shape[0]
    fresh = steps - 1
    piece = 256 if rows % 256 == 0 else rows

    def flush(c):
        return pltpu.make_async_copy(made_buf.at[c], res_ref.at[pl.ds(c * rows, rows), :], wrote.at[c])

    norm_copy = pltpu.make_async_copy(norm_buf, norm_ref, normed)

    def tail():
        coef = coef_ref[...]
        lefts = stat_ref[split : split + 8, 0:split]
        gains = dot(lefts, inverse_ref[...])
        errors = stat_ref[split : split + 8, split:] - dot(lefts, coef)
        yield
        done = []
        for j in reversed(range(fresh)):
            left = lefts[j : j + 1, :]
            k = gains[j : j + 1, :]
            d = errors[j : j + 1, :]
            for k0, s0, d0 in done:
                along = jnp.sum(k0 * left, axis=1, keepdims=True)
                k = k + k0 * (along / s0)
                d = d + along * d0
            s = 1.0 - jnp.sum(k * left, axis=1, keepdims=True)
            d = d / s
            done.append((k, s, d))
            yield
        pad7 = jnp.zeros((7, split), F32)
        kept = [coef]
        for k, _, d in done:
            turn = dot(jnp.concatenate([k, pad7], axis=0), jnp.concatenate([d, pad7], axis=0), ((0,), (0,)))
            kept.append(kept[-1] - turn)
        kept = kept[::-1]
        yield
        ftf, ftr = stat_ref[0:split, 0:split], stat_ref[0:split, split:]
        sq = stat_ref[split + 8 : split + 9, 0:split]
        curved = dot(ftf, jnp.concatenate(kept, axis=1))
        yield
        for j in range(steps):
            bent = kept[j] * (curved[:, j * split : (j + 1) * split] - 2.0 * ftr)
            norm_buf[j : j + 1, :] = (sq + jnp.sum(bent, axis=0, keepdims=True)) / total_rows
        norm_copy.start()

    stages = tail()
    wide = wide_ref[...]
    for c in range(chunks):
        for at in range(0, rows, piece):
            here = slice(c * rows + at, c * rows + at + piece)
            made = jnp.dot(pair[here, :], wide, preferred_element_type=F32)
            made_buf[c, at : at + piece, :] = rest[here, :] - (made[:, :split] + made[:, split:])
        next(stages, None)
        flush(c).start()
    for _ in stages:
        pass
    with jax.named_scope("flushwait"):
        for c in range(chunks):
            flush(c).wait()
        norm_copy.wait()


def on_device(axes, modes, points):
    n = axes[0][1] * axes[1][1]
    rows_dev, cols = modes.shape
    split = cols // 2
    npts = points.shape[0]
    steps = npts - PRIOR
    padded = -(-npts // 8) * 8
    count, _, _ = reducers_of(n, split // 8)
    deep = split // count
    vmem = pl.BlockSpec(memory_space=pltpu.VMEM)
    in_chunks = 6 if rows_dev % 96 == 0 else 1
    out_chunks = 12 if rows_dev % 96 == 0 else 1

    def sources(depth):
        return [pltpu.VMEM((count, depth, split), F32), pltpu.VMEM((n, depth, split), F32)]

    def paired(depth):
        return [
            pltpu.VMEM((2, count // 2, depth, split), F32),
            pltpu.VMEM((count // 2, depth, split), F32),
            pltpu.VMEM((n // 2, depth, split), F32),
        ]

    def sums(depth):
        return [pltpu.VMEM((depth, split), F32), pltpu.VMEM((count, depth, split), F32)]

    hbm = pl.BlockSpec(memory_space=pltpu.HBM)
    rest, pair, wide, coef, inverse, stat = pl.pallas_call(
        functools.partial(solve_kernel, axes, n),
        out_shape=[
            pltpu.VMEM((rows_dev + 8, split), F32),
            pltpu.VMEM((rows_dev, cols), BF16),
            pltpu.VMEM((cols, cols), BF16),
            pltpu.VMEM((split, split), F32),
            pltpu.VMEM((split, split), F32),
            pltpu.VMEM((split + 16, cols), F32),
        ],
        in_specs=[hbm] * 2,
        out_specs=[vmem] * 6,
        scratch_shapes=[
            pltpu.SMEM((npts,), jnp.int32),
            pltpu.SMEM((padded,), jnp.int32),
            pltpu.VMEM((rows_dev + 8, split), F32),
            pltpu.VMEM((split, rows_dev), BF16),
            pltpu.VMEM((2, padded // 8, 8, split), F32),
            pltpu.VMEM((2, split, cols), F32),
            pltpu.VMEM((2, cols, cols), F32),
            pltpu.VMEM((8, split), F32),
        ]
        + sources(deep)
        + sums(deep)
        + paired(deep)
        + sums(2 * deep)
        + paired(deep)
        + paired(deep + 1)
        + sums(deep + 1)
        + [pltpu.VMEM((split // 8, 8, split), F32), pltpu.VMEM((split // 8, 8, 8, split), F32)]
        + [pltpu.SemaphoreType.DMA]
        + [pltpu.SemaphoreType.DMA((in_chunks,))] * 2
        + [pltpu.SemaphoreType.DMA((20,))],
        compiler_params=pltpu.CompilerParams(
            collective_id=0, has_side_effects=True, vmem_limit_bytes=24 * 1024 * 1024
        ),
        name="solve",
    )(pltpu.with_memory_space_constraint(points, pltpu.HBM), pltpu.with_memory_space_constraint(modes, pltpu.HBM))
    residual, norms = pl.pallas_call(
        functools.partial(residual_kernel, rows_dev * n),
        out_shape=[
            jax.ShapeDtypeStruct((rows_dev, split), F32),
            jax.ShapeDtypeStruct((steps, split), F32),
        ],
        in_specs=[vmem] * 6,
        out_specs=[hbm, hbm],
        scratch_shapes=[
            pltpu.VMEM((out_chunks, rows_dev // out_chunks, split), F32),
            pltpu.VMEM((steps, split), F32),
            pltpu.SemaphoreType.DMA((out_chunks,)),
            pltpu.SemaphoreType.DMA,
        ],
        compiler_params=pltpu.CompilerParams(vmem_limit_bytes=16 * 1024 * 1024),
        name="residual",
    )(rest, pair, wide, coef, inverse, stat)
    return residual, norms


def solution(mesh):
    axes = tuple((name, mesh.shape[name]) for name in ("rows", "grp"))
    return jax.shard_map(
        functools.partial(on_device, axes),
        mesh=mesh,
        in_specs=(P(("rows", "grp"), None), P()),
        out_specs=(P(("rows", "grp"), None), P()),
        check_vma=False,
    )
```

```python
import functools

import jax
import jax.numpy as jnp
from jax import lax
from jax.experimental import pallas as pl
from jax.experimental.pallas import tpu as pltpu
from jax.sharding import PartitionSpec as P

PRIOR = 192
HOOK_REST, HOOK_FIT = 0, 8
WAVE = 1
UNROLL = 8
SEND_FIT = 2
HIGH = lax.Precision.HIGHEST
LOGICAL = pl.DeviceIdType.LOGICAL
F32 = jnp.float32
BF16 = jnp.bfloat16


def dot(a, b, dims=((1,), (0,))):
    return lax.dot_general(a, b, (dims, ((), ())), precision=HIGH, preferred_element_type=F32)


def halves(value):
    hi = value.astype(BF16)
    return hi, (value - hi.astype(F32)).astype(BF16)


def flat_index(axes):
    (first, _), (second, width) = axes
    return lax.axis_index(first) * width + lax.axis_index(second)


def small_inverse(e):
    size = len(e)
    e = [list(line) for line in e]
    for p in range(size):
        inv = 1.0 / e[p][p]
        line = [e[p][j] * inv for j in range(size)]
        line[p] = -inv
        for i in range(size):
            for j in range(i, size):
                if i == p or j == p:
                    continue
                e[i][j] = e[i][j] - e[p][i] * line[j]
                e[j][i] = e[i][j]
        for j in range(size):
            e[p][j] = line[j]
            e[j][p] = line[j]
    return [[-value for value in line] for line in e]


def added(terms):
    while len(terms) > 1:
        pairs = [terms[i] + terms[i + 1] for i in range(0, len(terms) - 1, 2)]
        terms = pairs + terms[len(pairs) * 2 :]
    return terms[0]


def sweep_inverse(gram, hook, line_ref, column_ref):
    size = gram.shape[0]
    steps = size // 8
    shape = (8, size)
    wide = (8, line_ref.shape[-1])
    tiles = [gram[8 * t : 8 * t + 8, :] for t in range(steps)]
    lane = lax.broadcasted_iota(jnp.int32, shape, 1)
    sub = lax.broadcasted_iota(jnp.int32, shape, 0)

    def column(tile, at):
        return jnp.broadcast_to(tile[:, at : at + 1], shape)

    for t in range(steps):
        k = 8 * t
        hook(k)
        own = [column(tiles[t], k + q) for q in range(8)]
        line_ref[t, :, 0:size] = tiles[t]
        for q in range(8):
            column_ref[t, q, :, 0:size] = own[q]
        entry = [[None] * 8 for _ in range(8)]
        for p in range(8):
            for q in range(p, 8):
                entry[p][q] = jnp.broadcast_to(column_ref[t, q, p : p + 1, 0:size], shape)
                entry[q][p] = entry[p][q]
        small = small_inverse(entry)
        inside = (lane >= k) & (lane < k + 8)
        rows = []
        for q in range(8):
            row = jnp.broadcast_to(line_ref[t, q : q + 1, 0:size], shape)
            rows.append(jnp.where(inside, jnp.where(lane == k + q, -1.0, 0.0), row))
        scaled = [added([small[p][q] * rows[q] for q in range(8)]) for p in range(8)]
        fresh = []
        for r in range(steps):
            columns = own if r == t else [column(tiles[r], k + p) for p in range(8)]
            value = jnp.where(inside, 0.0, tiles[r])
            fresh.append(value - added([columns[p] * scaled[p] for p in range(8)]))
        for p in range(8):
            fresh[t] = jnp.where(sub == p, scaled[p], fresh[t])
        tiles = fresh
    return -jnp.concatenate(tiles, axis=0)


def reducers_of(n, tiles):
    count = min(tiles // 2, n // 4)
    return count, n // 4 + 1, (n // 2) // count


def solve_kernel(
    axes, n, points_hbm, modes_ref, rest, pair, wide_ref, coef_ref, inverse_ref, stat_ref,
    points_ref, index_ref, fit, turned, picked, acc1, acc2, squares,
    part1, landed1, own1, full1, part2, mate2, landed2, own2, full2, part3, mate3, landed3, part4, mate4, landed4, own3, full3, own4, full4, line_ref, column_ref,
    listed, fit_in, rest_in, sems,
):
    me = flat_index(axes)
    rows_dev, cols = modes_ref.shape
    split = cols // 2
    npts = points_ref.shape[0]
    padded = index_ref.shape[0]
    chunks = fit_in.shape[0]
    rows = rows_dev // chunks
    count, first, stride = reducers_of(n, split // 8)
    deep = split // count
    mine = (me - first) // stride
    pairs = n // 2
    side = lax.rem(me, 2)
    partner = me + 1 - 2 * side
    (send1, recv1, share1, gather1, send2, recv2, share2, gather2, send3, recv3, send4, recv4, share3, gather3, share4, gather4) = [
        sems.at[i] for i in range(16)
    ]
    swaps = [(sems.at[16 + 2 * i], sems.at[17 + 2 * i]) for i in range(3)]
    reduces = (me >= first) & (me < first + count * stride) & (lax.rem(me - first + n, stride) == 0)

    def fetch_fit(c):
        at = pl.ds(c * rows, rows)
        return pltpu.make_async_copy(modes_ref.at[at, pl.ds(0, split)], fit.at[at, :], fit_in.at[c])

    def fetch_rest(c):
        at = pl.ds(c * rows, rows)
        return pltpu.make_async_copy(modes_ref.at[at, pl.ds(split, split)], rest.at[at, :], rest_in.at[c])

    def loop(body, start, stop, unroll=1):
        def step(i, carry):
            body(i)
            return carry

        lax.fori_loop(start, stop, step, 0, unroll=unroll)

    points_copy = pltpu.make_async_copy(points_hbm, points_ref, listed)
    points_copy.start()
    for c in range(chunks):
        fetch_fit(c).start()
    barrier = pltpu.get_barrier_semaphore()

    def greet(off):
        peer = lax.rem(me + off, n)
        pl.semaphore_signal(barrier, inc=1, device_id=peer, device_id_type=LOGICAL)

    loop(greet, 1, n)
    fit[rows_dev:, :] = jnp.zeros((8, split), F32)
    rest[rows_dev:, :] = jnp.zeros((8, split), F32)
    for total in (acc1, acc2, squares):
        total[...] = jnp.zeros_like(total)
    points_copy.wait()
    base = me * rows_dev

    def locate(i):
        at = points_ref[i] - base
        index_ref[i] = jnp.where((at >= 0) & (at < rows_dev), at, rows_dev)

    loop(locate, 0, npts, 4)
    for i in range(npts, padded):
        index_ref[i] = rows_dev

    wave = WAVE if chunks % WAVE == 0 else 1
    plain = (((1,), (0,)), ((), ()))

    def pieces_of(c):
        size = wave * rows // 2
        return [(i, slice(c * wave * rows + i * size, c * wave * rows + (i + 1) * size)) for i in range(2)]

    def fit_gram(c):
        for i, at in pieces_of(c):
            hi, lo = halves(fit[at, :])
            pair[at, :split] = hi
            pair[at, split:] = lo
            flip = hi.T
            turned[:, at] = flip
            acc1[i] += lax.dot_general(flip, jnp.concatenate([hi, lo], axis=1), plain, preferred_element_type=F32)

    def rest_gram(c):
        for i in range(wave):
            fetch_rest(c * wave + i).wait()
        for i, at in pieces_of(c):
            value = rest[at, :]
            hi, lo = halves(value)
            both = jnp.concatenate([turned[:, at], pair[at, split:].T], axis=0)
            acc2[i] += lax.dot_general(both, jnp.concatenate([hi, lo], axis=1), plain, preferred_element_type=F32)
            squares[...] += jnp.sum((value * value).reshape(-1, 8, split), axis=0)

    def take(source, half):
        def pick(t):
            for s in range(8):
                picked[half, t, s : s + 1, :] = source[pl.ds(index_ref[t * 8 + s], 1), :]

        loop(pick, 0, padded // 8)

    def peer_copy(src, dst, sent, got, peer):
        return pltpu.make_async_remote_copy(
            src_ref=src, dst_ref=dst, send_sem=sent, recv_sem=got,
            device_id=peer, device_id_type=LOGICAL,
        )

    def scatter(part, landed, sent, got):
        def body(off):
            i = lax.rem(me + 3 * off, count)
            peer = first + i * stride

            @pl.when(peer != me)
            def _():
                peer_copy(part.at[i], landed.at[me], sent, got, peer).start()

        loop(body, 0, count, UNROLL)

    def fill(part, value):
        for i in range(count):
            part[i % 2, i // 2, 0:deep, :] = value[i * deep : (i + 1) * deep, :]

    def swap(part, mate, sems_of):
        return peer_copy(part.at[1 - side], mate, *sems_of, partner)

    def scatter_pair(part, mate, landed, sems_of, sent, got):
        swap(part, mate, sems_of).wait_recv()
        part[side] = part[side] + mate[...]

        def body(off):
            i = lax.rem(me // 2 + off, count // 2)
            peer = first + (2 * i + side) * stride

            @pl.when(peer != me)
            def _():
                peer_copy(part.at[side, i], landed.at[me // 2], sent, got, peer).start()

        loop(body, 0, count // 2, UNROLL)

    local_pair = reduces & (lax.rem(mine + 2 * n, 2) == side)
    other_pair = reduces & (lax.rem(mine + 2 * n, 2) != side)

    def share(own, full, shared, gathered):
        full[mine] = own[...]

        def body(off):
            ahead = off + n // 4 - 1
            peer = lax.rem(me + jnp.where(ahead < n, ahead, ahead - n + 1), n)
            peer_copy(own, full.at[mine], shared, gathered, peer).start()

        loop(body, 1, n, UNROLL)

    def summed(landed):
        return added([landed[j] for j in range(landed.shape[0])])

    def reduce_all(part, landed, own, full, got, shared, gathered):
        @pl.when(reduces)
        def _():
            seen = landed.at[pl.ds(0, n - 1)]
            peer_copy(seen, seen, shared, got, me).wait_recv()
            landed[me] = part[mine]
            own[...] = summed(landed)
            share(own, full, shared, gathered)

    def reduce_pairs(pieces, own, full, shared, gathered):
        @pl.when(local_pair)
        def _():
            for part, landed, got in pieces:
                seen = landed.at[pl.ds(0, pairs - 1)]
                peer_copy(seen, seen, shared, got, me).wait_recv()
                landed[me // 2] = part[side, mine // 2]

        @pl.when(other_pair)
        def _():
            for part, landed, got in pieces:
                seen = landed.at[pl.ds(0, pairs)]
                peer_copy(seen, seen, shared, got, me).wait_recv()

        @pl.when(reduces)
        def _():
            at = 0
            for part, landed, got in pieces:
                own[at : at + landed.shape[1], :] = summed(landed)
                at += landed.shape[1]
            share(own, full, shared, gathered)

    def collect(full, shared, gathered):
        for held_here, size in ((reduces, count - 1), (jnp.logical_not(reduces), count)):

            @pl.when(held_here)
            def _():
                seen = full.at[pl.ds(0, size)]
                peer_copy(seen, seen, shared, gathered, me).wait_recv()

    def drain_shared(full, shared):
        @pl.when(reduces)
        def _():
            seen = full.at[pl.ds(0, count)]
            for _ in range((n - 1) // count):
                peer_copy(seen, seen, shared, shared, me).wait_send()
            rest_of = full.at[pl.ds(0, (n - 1) % count)]
            peer_copy(rest_of, rest_of, shared, shared, me).wait_send()

    def drain_sent(pieces, skips, size):
        for held_here, some in ((skips, size - 1), (jnp.logical_not(skips), size)):

            @pl.when(held_here)
            def _():
                for part, sent in pieces:
                    seen = part.at[pl.ds(0, some)]
                    peer_copy(seen, seen, sent, sent, me).wait_send()

    waves = chunks // wave
    with jax.named_scope("fgram"):
        for c in range(waves):
            for i in range(wave):
                fetch_fit(c * wave + i).wait()
            if c == max(waves - 3, 0):
                for i in range(chunks):
                    fetch_rest(i).start()
            if c < waves - 1:
                fit_gram(c)
    with jax.named_scope("fpick"):
        take(fit, 0)
    with jax.named_scope("fdot"):
        left = picked[0].reshape(padded, split)
        part1[...] = dot(left, left, ((0,), (0,))).reshape(part1.shape)
    with jax.named_scope("barrier"):
        pl.semaphore_wait(barrier, n - 1)
    with jax.named_scope("scat1"):
        scatter(part1, landed1, send1, recv1)

    with jax.named_scope("fgram2"):
        fit_gram(waves - 1)
        total = acc1[0] + acc1[1]
        cross = total[:, split:]
        fill(part2, total[:, :split] + (cross + cross.T))
        swap(part2, mate2, swaps[0]).start()
    for c in range(waves):
        with jax.named_scope("rgram"):
            rest_gram(c)
        if c == SEND_FIT:
            with jax.named_scope("scat2"):
                scatter_pair(part2, mate2, landed2, swaps[0], send2, recv2)
    with jax.named_scope("swap3"):
        total = acc2[0] + acc2[1]
        fill(part3, total[:split, :split] + (total[:split, split:] + total[split:, :split]))
        swap(part3, mate3, swaps[1]).start()
    with jax.named_scope("rpick"):
        take(rest, 1)
    with jax.named_scope("rdot"):
        fresh = npts - PRIOR - 1
        tail = slice(deep, deep + 1)
        part4[:, :, tail, :] = jnp.zeros((2, count // 2, 1, split), F32)
        fill(part4, dot(picked[0].reshape(padded, split), picked[1].reshape(padded, split), ((0,), (0,))))
        for i in range(fresh):
            for side_of in range(2):
                at = PRIOR + 1 + i
                part4[side_of, i, tail, :] = picked[side_of, at // 8, at % 8 : at % 8 + 1, :]
        part4[0, fresh, tail, :] = jnp.sum(squares[...], axis=0, keepdims=True)
        swap(part4, mate4, swaps[2]).start()
    with jax.named_scope("scat3"):
        scatter_pair(part3, mate3, landed3, swaps[1], send3, recv3)
    with jax.named_scope("scat4"):
        scatter_pair(part4, mate4, landed4, swaps[2], send4, recv4)

    with jax.named_scope("red1"):
        reduce_all(part1, landed1, own1, full1, recv1, share1, gather1)
    with jax.named_scope("red2"):
        reduce_pairs([(part2, landed2, recv2)], own2, full2, share2, gather2)
    with jax.named_scope("col1"):
        collect(full1, share1, gather1)

    half = split // 2

    def hook(k):
        if k == HOOK_REST:
            with jax.named_scope("red3"):
                reduce_pairs([(part4, landed4, recv4)], own3, full3, share3, gather3)
        if k == HOOK_FIT:
            with jax.named_scope("red4"):
                reduce_pairs([(part3, landed3, recv3)], own4, full4, share4, gather4)

    with jax.named_scope("sweepP"):
        gram = full1[...].reshape(split, split)
        upper = sweep_inverse(gram[:half, :half], hook, line_ref, column_ref)
    with jax.named_scope("mid"):
        corner = gram[:half, half:]
        link = dot(upper, corner)
        schur = gram[half:, half:] - dot(corner, link, ((0,), (0,)))
    with jax.named_scope("sweepZ"):
        later = pl.ds(half // 8, half // 8)
        lower = sweep_inverse(schur, lambda k: None, line_ref.at[later], column_ref.at[later])
    with jax.named_scope("join"):
        bridge = dot(link, lower)
        above = jnp.concatenate([upper + dot(bridge, link, ((1,), (1,))), -bridge], axis=1)
        inverse = jnp.concatenate([above, jnp.concatenate([-bridge.T, lower], axis=1)], axis=0)
        inverse_ref[...] = inverse
    with jax.named_scope("col3"):
        collect(full3, share3, gather3)
    with jax.named_scope("coef"):
        coef = dot(inverse, full3[:, 0:deep, :].reshape(split, split))
        c_hi, c_lo = halves(coef)
        wide_ref[0:split, 0:split] = c_hi
        wide_ref[split:, 0:split] = c_hi
        wide_ref[0:split, split:] = c_lo
        wide_ref[split:, split:] = jnp.zeros((split, split), BF16)
        coef_ref[...] = coef
        zero = jnp.zeros((8 - fresh, split), F32)
        for part in range(2):
            lines = [full3[2 * i + part, tail, :] for i in range(fresh)]
            stat_ref[split : split + 8, part * split : (part + 1) * split] = jnp.concatenate(lines + [zero], axis=0)
        stat_ref[split + 8 :, 0:split] = jnp.broadcast_to(full3[2 * fresh, tail, :], (8, split))
        stat_ref[split + 8 :, split:] = jnp.zeros((8, split), F32)
    with jax.named_scope("col2"):
        collect(full2, share2, gather2)
        stat_ref[0:split, 0:split] = full2[...].reshape(split, split)
        collect(full4, share4, gather4)
        stat_ref[0:split, split:] = full4[...].reshape(split, split)
    with jax.named_scope("drain"):
        drain_sent([(part1, send1)], reduces, count)
        drain_sent([(mate2, send2), (mate3, send3), (mate4, send4)], local_pair, count // 2)
        for part, mate, sems_of in ((part2, mate2, swaps[0]), (part3, mate3, swaps[1]), (part4, mate4, swaps[2])):
            swap(part, mate, sems_of).wait_send()
        for full, shared in ((full1, share1), (full2, share2), (full3, share3), (full4, share4)):
            drain_shared(full, shared)


def residual_kernel(
    total_rows, rest, pair, wide_ref, coef_ref, inverse_ref, stat_ref, res_ref, norm_ref, made_buf, norm_buf, wrote, normed
):
    chunks, rows, split = made_buf.shape
    steps = norm_buf.shape[0]
    fresh = steps - 1
    piece = 256 if rows % 256 == 0 else rows

    def flush(c):
        return pltpu.make_async_copy(made_buf.at[c], res_ref.at[pl.ds(c * rows, rows), :], wrote.at[c])

    norm_copy = pltpu.make_async_copy(norm_buf, norm_ref, normed)

    def tail():
        coef = coef_ref[...]
        lefts = stat_ref[split : split + 8, 0:split]
        gains = dot(lefts, inverse_ref[...])
        errors = stat_ref[split : split + 8, split:] - dot(lefts, coef)
        yield
        done = []
        for j in reversed(range(fresh)):
            left = lefts[j : j + 1, :]
            k = gains[j : j + 1, :]
            d = errors[j : j + 1, :]
            for k0, s0, d0 in done:
                along = jnp.sum(k0 * left, axis=1, keepdims=True)
                k = k + k0 * (along / s0)
                d = d + along * d0
            s = 1.0 - jnp.sum(k * left, axis=1, keepdims=True)
            d = d / s
            done.append((k, s, d))
            yield
        pad7 = jnp.zeros((7, split), F32)
        kept = [coef]
        for k, _, d in done:
            turn = dot(jnp.concatenate([k, pad7], axis=0), jnp.concatenate([d, pad7], axis=0), ((0,), (0,)))
            kept.append(kept[-1] - turn)
        kept = kept[::-1]
        yield
        ftf, ftr = stat_ref[0:split, 0:split], stat_ref[0:split, split:]
        sq = stat_ref[split + 8 : split + 9, 0:split]
        curved = dot(ftf, jnp.concatenate(kept, axis=1))
        yield
        for j in range(steps):
            bent = kept[j] * (curved[:, j * split : (j + 1) * split] - 2.0 * ftr)
            norm_buf[j : j + 1, :] = (sq + jnp.sum(bent, axis=0, keepdims=True)) / total_rows
        norm_copy.start()

    stages = tail()
    wide = wide_ref[...]
    for c in range(chunks):
        for at in range(0, rows, piece):
            here = slice(c * rows + at, c * rows + at + piece)
            made = jnp.dot(pair[here, :], wide, preferred_element_type=F32)
            made_buf[c, at : at + piece, :] = rest[here, :] - (made[:, :split] + made[:, split:])
        next(stages, None)
        flush(c).start()
    for _ in stages:
        pass
    with jax.named_scope("flushwait"):
        for c in range(chunks):
            flush(c).wait()
        norm_copy.wait()


def on_device(axes, modes, points):
    n = axes[0][1] * axes[1][1]
    rows_dev, cols = modes.shape
    split = cols // 2
    npts = points.shape[0]
    steps = npts - PRIOR
    padded = -(-npts // 8) * 8
    count, _, _ = reducers_of(n, split // 8)
    deep = split // count
    vmem = pl.BlockSpec(memory_space=pltpu.VMEM)
    in_chunks = 6 if rows_dev % 96 == 0 else 1
    out_chunks = 12 if rows_dev % 96 == 0 else 1

    def sources(depth):
        return [pltpu.VMEM((count, depth, split), F32), pltpu.VMEM((n, depth, split), F32)]

    def paired(depth):
        return [
            pltpu.VMEM((2, count // 2, depth, split), F32),
            pltpu.VMEM((count // 2, depth, split), F32),
            pltpu.VMEM((n // 2, depth, split), F32),
        ]

    def sums(depth):
        return [pltpu.VMEM((depth, split), F32), pltpu.VMEM((count, depth, split), F32)]

    hbm = pl.BlockSpec(memory_space=pltpu.HBM)
    rest, pair, wide, coef, inverse, stat = pl.pallas_call(
        functools.partial(solve_kernel, axes, n),
        out_shape=[
            pltpu.VMEM((rows_dev + 8, split), F32),
            pltpu.VMEM((rows_dev, cols), BF16),
            pltpu.VMEM((cols, cols), BF16),
            pltpu.VMEM((split, split), F32),
            pltpu.VMEM((split, split), F32),
            pltpu.VMEM((split + 16, cols), F32),
        ],
        in_specs=[hbm] * 2,
        out_specs=[vmem] * 6,
        scratch_shapes=[
            pltpu.SMEM((npts,), jnp.int32),
            pltpu.SMEM((padded,), jnp.int32),
            pltpu.VMEM((rows_dev + 8, split), F32),
            pltpu.VMEM((split, rows_dev), BF16),
            pltpu.VMEM((2, padded // 8, 8, split), F32),
            pltpu.VMEM((2, split, cols), F32),
            pltpu.VMEM((2, cols, cols), F32),
            pltpu.VMEM((8, split), F32),
        ]
        + sources(deep)
        + sums(deep)
        + paired(deep)
        + sums(deep)
        + paired(deep)
        + paired(deep + 1)
        + sums(deep + 1)
        + sums(deep)
        + [pltpu.VMEM((split // 8, 8, split), F32), pltpu.VMEM((split // 8, 8, 8, split), F32)]
        + [pltpu.SemaphoreType.DMA]
        + [pltpu.SemaphoreType.DMA((in_chunks,))] * 2
        + [pltpu.SemaphoreType.DMA((22,))],
        compiler_params=pltpu.CompilerParams(
            collective_id=0, has_side_effects=True, vmem_limit_bytes=24 * 1024 * 1024
        ),
        name="solve",
    )(pltpu.with_memory_space_constraint(points, pltpu.HBM), pltpu.with_memory_space_constraint(modes, pltpu.HBM))
    residual, norms = pl.pallas_call(
        functools.partial(residual_kernel, rows_dev * n),
        out_shape=[
            jax.ShapeDtypeStruct((rows_dev, split), F32),
            jax.ShapeDtypeStruct((steps, split), F32),
        ],
        in_specs=[vmem] * 6,
        out_specs=[hbm, hbm],
        scratch_shapes=[
            pltpu.VMEM((out_chunks, rows_dev // out_chunks, split), F32),
            pltpu.VMEM((steps, split), F32),
            pltpu.SemaphoreType.DMA((out_chunks,)),
            pltpu.SemaphoreType.DMA,
        ],
        compiler_params=pltpu.CompilerParams(vmem_limit_bytes=16 * 1024 * 1024),
        name="residual",
    )(rest, pair, wide, coef, inverse, stat)
    return residual, norms


def solution(mesh):
    axes = tuple((name, mesh.shape[name]) for name in ("rows", "grp"))
    return jax.shard_map(
        functools.partial(on_device, axes),
        mesh=mesh,
        in_specs=(P(("rows", "grp"), None), P()),
        out_specs=(P(("rows", "grp"), None), P()),
        check_vma=False,
    )
```

```python
import functools

import jax
import jax.numpy as jnp
from jax import lax
from jax.experimental import pallas as pl
from jax.experimental.pallas import tpu as pltpu
from jax.sharding import PartitionSpec as P

PRIOR = 192
HOOK_REST, HOOK_FIT = 0, 8
WAVE = 1
UNROLL = 8
SEND_FIT = 2
HIGH = lax.Precision.HIGHEST
LOGICAL = pl.DeviceIdType.LOGICAL
F32 = jnp.float32
BF16 = jnp.bfloat16


def dot(a, b, dims=((1,), (0,))):
    return lax.dot_general(a, b, (dims, ((), ())), precision=HIGH, preferred_element_type=F32)


def halves(value):
    hi = value.astype(BF16)
    return hi, (value - hi.astype(F32)).astype(BF16)


def flat_index(axes):
    (first, _), (second, width) = axes
    return lax.axis_index(first) * width + lax.axis_index(second)


def small_inverse(e):
    size = len(e)
    e = [list(line) for line in e]
    for p in range(size):
        inv = 1.0 / e[p][p]
        line = [e[p][j] * inv for j in range(size)]
        line[p] = -inv
        for i in range(size):
            for j in range(i, size):
                if i == p or j == p:
                    continue
                e[i][j] = e[i][j] - e[p][i] * line[j]
                e[j][i] = e[i][j]
        for j in range(size):
            e[p][j] = line[j]
            e[j][p] = line[j]
    return [[-value for value in line] for line in e]


def added(terms):
    while len(terms) > 1:
        pairs = [terms[i] + terms[i + 1] for i in range(0, len(terms) - 1, 2)]
        terms = pairs + terms[len(pairs) * 2 :]
    return terms[0]


def sweep_inverse(gram, hook, line_ref, column_ref):
    size = gram.shape[0]
    steps = size // 8
    shape = (8, size)
    wide = (8, line_ref.shape[-1])
    tiles = [gram[8 * t : 8 * t + 8, :] for t in range(steps)]
    lane = lax.broadcasted_iota(jnp.int32, shape, 1)
    sub = lax.broadcasted_iota(jnp.int32, shape, 0)

    def column(tile, at):
        return jnp.broadcast_to(tile[:, at : at + 1], shape)

    for t in range(steps):
        k = 8 * t
        hook(k)
        own = [column(tiles[t], k + q) for q in range(8)]
        line_ref[t, :, 0:size] = tiles[t]
        for q in range(8):
            column_ref[t, q, :, 0:size] = own[q]
        entry = [[None] * 8 for _ in range(8)]
        for p in range(8):
            for q in range(p, 8):
                entry[p][q] = jnp.broadcast_to(column_ref[t, q, p : p + 1, 0:size], shape)
                entry[q][p] = entry[p][q]
        small = small_inverse(entry)
        inside = (lane >= k) & (lane < k + 8)
        rows = []
        for q in range(8):
            row = jnp.broadcast_to(line_ref[t, q : q + 1, 0:size], shape)
            rows.append(jnp.where(inside, jnp.where(lane == k + q, -1.0, 0.0), row))
        scaled = [added([small[p][q] * rows[q] for q in range(8)]) for p in range(8)]
        fresh = []
        for r in range(steps):
            columns = own if r == t else [column(tiles[r], k + p) for p in range(8)]
            value = jnp.where(inside, 0.0, tiles[r])
            fresh.append(value - added([columns[p] * scaled[p] for p in range(8)]))
        for p in range(8):
            fresh[t] = jnp.where(sub == p, scaled[p], fresh[t])
        tiles = fresh
    return -jnp.concatenate(tiles, axis=0)


def reducers_of(n, tiles):
    count = min(tiles // 2, n // 4)
    return count, n // 4 + 1, (n // 2) // count


def solve_kernel(
    axes, n, points_hbm, modes_ref, rest, pair, wide_ref, coef_ref, inverse_ref, stat_ref,
    points_ref, index_ref, fit, turned, picked, acc1, acc2, squares,
    part1, landed1, own1, full1, part2, mate2, landed2, own2, full2, part3, mate3, landed3, part4, mate4, landed4, own3, full3, own4, full4, line_ref, column_ref,
    listed, fit_in, rest_in, sems,
):
    me = flat_index(axes)
    rows_dev, cols = modes_ref.shape
    split = cols // 2
    npts = points_ref.shape[0]
    padded = index_ref.shape[0]
    chunks = fit_in.shape[0]
    rows = rows_dev // chunks
    count, first, stride = reducers_of(n, split // 8)
    deep = split // count
    mine = (me - first) // stride
    pairs = n // 2
    side = lax.rem(me, 2)
    partner = me + 1 - 2 * side
    (send1, recv1, share1, gather1, send2, recv2, share2, gather2, send3, recv3, send4, recv4, share3, gather3, share4, gather4) = [
        sems.at[i] for i in range(16)
    ]
    swaps = [(sems.at[16 + 2 * i], sems.at[17 + 2 * i]) for i in range(3)]
    reduces = (me >= first) & (me < first + count * stride) & (lax.rem(me - first + n, stride) == 0)

    def fetch_fit(c):
        at = pl.ds(c * rows, rows)
        return pltpu.make_async_copy(modes_ref.at[at, pl.ds(0, split)], fit.at[at, :], fit_in.at[c])

    def fetch_rest(c):
        at = pl.ds(c * rows, rows)
        return pltpu.make_async_copy(modes_ref.at[at, pl.ds(split, split)], rest.at[at, :], rest_in.at[c])

    def loop(body, start, stop, unroll=1):
        def step(i, carry):
            body(i)
            return carry

        lax.fori_loop(start, stop, step, 0, unroll=unroll)

    points_copy = pltpu.make_async_copy(points_hbm, points_ref, listed)
    points_copy.start()
    for c in range(chunks):
        fetch_fit(c).start()
    barrier = pltpu.get_barrier_semaphore()

    def greet(off):
        peer = lax.rem(me + off, n)
        pl.semaphore_signal(barrier, inc=1, device_id=peer, device_id_type=LOGICAL)

    loop(greet, 1, n)
    fit[rows_dev:, :] = jnp.zeros((8, split), F32)
    rest[rows_dev:, :] = jnp.zeros((8, split), F32)
    for total in (acc1, acc2, squares):
        total[...] = jnp.zeros_like(total)
    points_copy.wait()
    base = me * rows_dev

    def locate(i):
        at = points_ref[i] - base
        index_ref[i] = jnp.where((at >= 0) & (at < rows_dev), at, rows_dev)

    loop(locate, 0, npts, 4)
    for i in range(npts, padded):
        index_ref[i] = rows_dev

    wave = WAVE if chunks % WAVE == 0 else 1
    plain = (((1,), (0,)), ((), ()))

    def pieces_of(c):
        size = wave * rows // 2
        return [(i, slice(c * wave * rows + i * size, c * wave * rows + (i + 1) * size)) for i in range(2)]

    def fit_gram(c):
        for i, at in pieces_of(c):
            hi, lo = halves(fit[at, :])
            pair[at, :split] = hi
            pair[at, split:] = lo
            flip = hi.T
            turned[:, at] = flip
            acc1[i] += lax.dot_general(flip, jnp.concatenate([hi, lo], axis=1), plain, preferred_element_type=F32)

    def rest_gram(c):
        for i in range(wave):
            fetch_rest(c * wave + i).wait()
        for i, at in pieces_of(c):
            value = rest[at, :]
            hi, lo = halves(value)
            both = jnp.concatenate([turned[:, at], pair[at, split:].T], axis=0)
            acc2[i] += lax.dot_general(both, jnp.concatenate([hi, lo], axis=1), plain, preferred_element_type=F32)
            squares[...] += jnp.sum((value * value).reshape(-1, 8, split), axis=0)

    def take(source, half):
        def pick(t):
            for s in range(8):
                picked[half, t, s : s + 1, :] = source[pl.ds(index_ref[t * 8 + s], 1), :]

        loop(pick, 0, padded // 8)

    def peer_copy(src, dst, sent, got, peer):
        return pltpu.make_async_remote_copy(
            src_ref=src, dst_ref=dst, send_sem=sent, recv_sem=got,
            device_id=peer, device_id_type=LOGICAL,
        )

    def scatter(part, landed, sent, got):
        def body(off):
            i = lax.rem(me + 3 * off, count)
            peer = first + i * stride

            @pl.when(peer != me)
            def _():
                peer_copy(part.at[i], landed.at[me], sent, got, peer).start()

        loop(body, 0, count, UNROLL)

    def fill(part, value):
        for i in range(count):
            part[i % 2, i // 2, 0:deep, :] = value[i * deep : (i + 1) * deep, :]

    def swap(part, mate, sems_of):
        return peer_copy(part.at[1 - side], mate, *sems_of, partner)

    def scatter_pair(part, mate, landed, sems_of, sent, got):
        swap(part, mate, sems_of).wait_recv()
        part[side] = part[side] + mate[...]

        def body(off):
            i = lax.rem(me // 2 + off, count // 2)
            peer = first + (2 * i + side) * stride

            @pl.when(peer != me)
            def _():
                peer_copy(part.at[side, i], landed.at[me // 2], sent, got, peer).start()

        loop(body, 0, count // 2, UNROLL)

    local_pair = reduces & (lax.rem(mine + 2 * n, 2) == side)
    other_pair = reduces & (lax.rem(mine + 2 * n, 2) != side)

    def share(own, full, shared, gathered, skip=0):
        full[mine] = own[...]

        def body(off):
            ahead = off + max(skip, 1)
            peer = lax.rem(me + jnp.where(ahead < n, ahead, ahead - n + 1), n)
            peer_copy(own, full.at[mine], shared, gathered, peer).start()

        loop(body, 1, n, UNROLL)

    def summed(landed):
        return added([landed[j] for j in range(landed.shape[0])])

    def reduce_all(part, landed, own, full, got, shared, gathered):
        @pl.when(reduces)
        def _():
            seen = landed.at[pl.ds(0, n - 1)]
            peer_copy(seen, seen, shared, got, me).wait_recv()
            landed[me] = part[mine]
            own[...] = summed(landed)
            share(own, full, shared, gathered, n // 4 - 1)

    def reduce_pairs(pieces, own, full, shared, gathered):
        @pl.when(local_pair)
        def _():
            for part, landed, got in pieces:
                seen = landed.at[pl.ds(0, pairs - 1)]
                peer_copy(seen, seen, shared, got, me).wait_recv()
                landed[me // 2] = part[side, mine // 2]

        @pl.when(other_pair)
        def _():
            for part, landed, got in pieces:
                seen = landed.at[pl.ds(0, pairs)]
                peer_copy(seen, seen, shared, got, me).wait_recv()

        @pl.when(reduces)
        def _():
            at = 0
            for part, landed, got in pieces:
                own[at : at + landed.shape[1], :] = summed(landed)
                at += landed.shape[1]
            share(own, full, shared, gathered)

    def collect(full, shared, gathered):
        for held_here, size in ((reduces, count - 1), (jnp.logical_not(reduces), count)):

            @pl.when(held_here)
            def _():
                seen = full.at[pl.ds(0, size)]
                peer_copy(seen, seen, shared, gathered, me).wait_recv()

    def drain_shared(full, shared):
        @pl.when(reduces)
        def _():
            seen = full.at[pl.ds(0, count)]
            for _ in range((n - 1) // count):
                peer_copy(seen, seen, shared, shared, me).wait_send()
            rest_of = full.at[pl.ds(0, (n - 1) % count)]
            peer_copy(rest_of, rest_of, shared, shared, me).wait_send()

    def drain_sent(pieces, skips, size):
        for held_here, some in ((skips, size - 1), (jnp.logical_not(skips), size)):

            @pl.when(held_here)
            def _():
                for part, sent in pieces:
                    seen = part.at[pl.ds(0, some)]
                    peer_copy(seen, seen, sent, sent, me).wait_send()

    waves = chunks // wave
    with jax.named_scope("fgram"):
        for c in range(waves):
            for i in range(wave):
                fetch_fit(c * wave + i).wait()
            if c == max(waves - 3, 0):
                for i in range(chunks):
                    fetch_rest(i).start()
            if c < waves - 1:
                fit_gram(c)
    with jax.named_scope("fpick"):
        take(fit, 0)
    with jax.named_scope("fdot"):
        left = picked[0].reshape(padded, split)
        part1[...] = dot(left, left, ((0,), (0,))).reshape(part1.shape)
    with jax.named_scope("barrier"):
        pl.semaphore_wait(barrier, n - 1)
    with jax.named_scope("scat1"):
        scatter(part1, landed1, send1, recv1)

    with jax.named_scope("fgram2"):
        fit_gram(waves - 1)
        total = acc1[0] + acc1[1]
        cross = total[:, split:]
        fill(part2, total[:, :split] + (cross + cross.T))
        swap(part2, mate2, swaps[0]).start()
    for c in range(waves):
        with jax.named_scope("rgram"):
            rest_gram(c)
        if c == SEND_FIT:
            with jax.named_scope("scat2"):
                scatter_pair(part2, mate2, landed2, swaps[0], send2, recv2)
    with jax.named_scope("swap3"):
        total = acc2[0] + acc2[1]
        fill(part3, total[:split, :split] + (total[:split, split:] + total[split:, :split]))
        swap(part3, mate3, swaps[1]).start()
    with jax.named_scope("rpick"):
        take(rest, 1)
    with jax.named_scope("rdot"):
        fresh = npts - PRIOR - 1
        tail = slice(deep, deep + 1)
        part4[:, :, tail, :] = jnp.zeros((2, count // 2, 1, split), F32)
        fill(part4, dot(picked[0].reshape(padded, split), picked[1].reshape(padded, split), ((0,), (0,))))
        for i in range(fresh):
            for side_of in range(2):
                at = PRIOR + 1 + i
                part4[side_of, i, tail, :] = picked[side_of, at // 8, at % 8 : at % 8 + 1, :]
        part4[0, fresh, tail, :] = jnp.sum(squares[...], axis=0, keepdims=True)
        swap(part4, mate4, swaps[2]).start()
    with jax.named_scope("scat3"):
        scatter_pair(part3, mate3, landed3, swaps[1], send3, recv3)
    with jax.named_scope("scat4"):
        scatter_pair(part4, mate4, landed4, swaps[2], send4, recv4)

    with jax.named_scope("red1"):
        reduce_all(part1, landed1, own1, full1, recv1, share1, gather1)
    with jax.named_scope("red2"):
        reduce_pairs([(part2, landed2, recv2)], own2, full2, share2, gather2)
    with jax.named_scope("col1"):
        collect(full1, share1, gather1)

    half = split // 2

    def hook(k):
        if k == HOOK_REST:
            with jax.named_scope("red3"):
                reduce_pairs([(part4, landed4, recv4)], own3, full3, share3, gather3)
        if k == HOOK_FIT:
            with jax.named_scope("red4"):
                reduce_pairs([(part3, landed3, recv3)], own4, full4, share4, gather4)

    with jax.named_scope("sweepP"):
        gram = full1[...].reshape(split, split)
        upper = sweep_inverse(gram[:half, :half], hook, line_ref, column_ref)
    with jax.named_scope("mid"):
        corner = gram[:half, half:]
        link = dot(upper, corner)
        schur = gram[half:, half:] - dot(corner, link, ((0,), (0,)))
    with jax.named_scope("sweepZ"):
        later = pl.ds(half // 8, half // 8)
        lower = sweep_inverse(schur, lambda k: None, line_ref.at[later], column_ref.at[later])
    with jax.named_scope("join"):
        bridge = dot(link, lower)
        above = jnp.concatenate([upper + dot(bridge, link, ((1,), (1,))), -bridge], axis=1)
        inverse = jnp.concatenate([above, jnp.concatenate([-bridge.T, lower], axis=1)], axis=0)
        inverse_ref[...] = inverse
    with jax.named_scope("col3"):
        collect(full3, share3, gather3)
    with jax.named_scope("coef"):
        coef = dot(inverse, full3[:, 0:deep, :].reshape(split, split))
        c_hi, c_lo = halves(coef)
        wide_ref[0:split, 0:split] = c_hi
        wide_ref[split:, 0:split] = c_hi
        wide_ref[0:split, split:] = c_lo
        wide_ref[split:, split:] = jnp.zeros((split, split), BF16)
        coef_ref[...] = coef
        zero = jnp.zeros((8 - fresh, split), F32)
        for part in range(2):
            lines = [full3[2 * i + part, tail, :] for i in range(fresh)]
            stat_ref[split : split + 8, part * split : (part + 1) * split] = jnp.concatenate(lines + [zero], axis=0)
        stat_ref[split + 8 :, 0:split] = jnp.broadcast_to(full3[2 * fresh, tail, :], (8, split))
        stat_ref[split + 8 :, split:] = jnp.zeros((8, split), F32)
    with jax.named_scope("col2"):
        collect(full2, share2, gather2)
        stat_ref[0:split, 0:split] = full2[...].reshape(split, split)
        collect(full4, share4, gather4)
        stat_ref[0:split, split:] = full4[...].reshape(split, split)
    with jax.named_scope("drain"):
        drain_sent([(part1, send1)], reduces, count)
        drain_sent([(mate2, send2), (mate3, send3), (mate4, send4)], local_pair, count // 2)
        for part, mate, sems_of in ((part2, mate2, swaps[0]), (part3, mate3, swaps[1]), (part4, mate4, swaps[2])):
            swap(part, mate, sems_of).wait_send()
        for full, shared in ((full1, share1), (full2, share2), (full3, share3), (full4, share4)):
            drain_shared(full, shared)


def residual_kernel(
    total_rows, rest, pair, wide_ref, coef_ref, inverse_ref, stat_ref, res_ref, norm_ref, made_buf, norm_buf, wrote, normed
):
    chunks, rows, split = made_buf.shape
    steps = norm_buf.shape[0]
    fresh = steps - 1
    piece = 256 if rows % 256 == 0 else rows

    def flush(c):
        return pltpu.make_async_copy(made_buf.at[c], res_ref.at[pl.ds(c * rows, rows), :], wrote.at[c])

    norm_copy = pltpu.make_async_copy(norm_buf, norm_ref, normed)

    def tail():
        coef = coef_ref[...]
        lefts = stat_ref[split : split + 8, 0:split]
        gains = dot(lefts, inverse_ref[...])
        errors = stat_ref[split : split + 8, split:] - dot(lefts, coef)
        yield
        done = []
        for j in reversed(range(fresh)):
            left = lefts[j : j + 1, :]
            k = gains[j : j + 1, :]
            d = errors[j : j + 1, :]
            for k0, s0, d0 in done:
                along = jnp.sum(k0 * left, axis=1, keepdims=True)
                k = k + k0 * (along / s0)
                d = d + along * d0
            s = 1.0 - jnp.sum(k * left, axis=1, keepdims=True)
            d = d / s
            done.append((k, s, d))
            yield
        pad7 = jnp.zeros((7, split), F32)
        kept = [coef]
        for k, _, d in done:
            turn = dot(jnp.concatenate([k, pad7], axis=0), jnp.concatenate([d, pad7], axis=0), ((0,), (0,)))
            kept.append(kept[-1] - turn)
        kept = kept[::-1]
        yield
        ftf, ftr = stat_ref[0:split, 0:split], stat_ref[0:split, split:]
        sq = stat_ref[split + 8 : split + 9, 0:split]
        curved = dot(ftf, jnp.concatenate(kept, axis=1))
        yield
        for j in range(steps):
            bent = kept[j] * (curved[:, j * split : (j + 1) * split] - 2.0 * ftr)
            norm_buf[j : j + 1, :] = (sq + jnp.sum(bent, axis=0, keepdims=True)) / total_rows
        norm_copy.start()

    stages = tail()
    wide = wide_ref[...]
    for c in range(chunks):
        for at in range(0, rows, piece):
            here = slice(c * rows + at, c * rows + at + piece)
            made = jnp.dot(pair[here, :], wide, preferred_element_type=F32)
            made_buf[c, at : at + piece, :] = rest[here, :] - (made[:, :split] + made[:, split:])
        next(stages, None)
        flush(c).start()
    for _ in stages:
        pass
    with jax.named_scope("flushwait"):
        for c in range(chunks):
            flush(c).wait()
        norm_copy.wait()


def on_device(axes, modes, points):
    n = axes[0][1] * axes[1][1]
    rows_dev, cols = modes.shape
    split = cols // 2
    npts = points.shape[0]
    steps = npts - PRIOR
    padded = -(-npts // 8) * 8
    count, _, _ = reducers_of(n, split // 8)
    deep = split // count
    vmem = pl.BlockSpec(memory_space=pltpu.VMEM)
    in_chunks = 6 if rows_dev % 96 == 0 else 1
    out_chunks = 6 if rows_dev % 96 == 0 else 1

    def sources(depth):
        return [pltpu.VMEM((count, depth, split), F32), pltpu.VMEM((n, depth, split), F32)]

    def paired(depth):
        return [
            pltpu.VMEM((2, count // 2, depth, split), F32),
            pltpu.VMEM((count // 2, depth, split), F32),
            pltpu.VMEM((n // 2, depth, split), F32),
        ]

    def sums(depth):
        return [pltpu.VMEM((depth, split), F32), pltpu.VMEM((count, depth, split), F32)]

    hbm = pl.BlockSpec(memory_space=pltpu.HBM)
    rest, pair, wide, coef, inverse, stat = pl.pallas_call(
        functools.partial(solve_kernel, axes, n),
        out_shape=[
            pltpu.VMEM((rows_dev + 8, split), F32),
            pltpu.VMEM((rows_dev, cols), BF16),
            pltpu.VMEM((cols, cols), BF16),
            pltpu.VMEM((split, split), F32),
            pltpu.VMEM((split, split), F32),
            pltpu.VMEM((split + 16, cols), F32),
        ],
        in_specs=[hbm] * 2,
        out_specs=[vmem] * 6,
        scratch_shapes=[
            pltpu.SMEM((npts,), jnp.int32),
            pltpu.SMEM((padded,), jnp.int32),
            pltpu.VMEM((rows_dev + 8, split), F32),
            pltpu.VMEM((split, rows_dev), BF16),
            pltpu.VMEM((2, padded // 8, 8, split), F32),
            pltpu.VMEM((2, split, cols), F32),
            pltpu.VMEM((2, cols, cols), F32),
            pltpu.VMEM((8, split), F32),
        ]
        + sources(deep)
        + sums(deep)
        + paired(deep)
        + sums(deep)
        + paired(deep)
        + paired(deep + 1)
        + sums(deep + 1)
        + sums(deep)
        + [pltpu.VMEM((split // 8, 8, split), F32), pltpu.VMEM((split // 8, 8, 8, split), F32)]
        + [pltpu.SemaphoreType.DMA]
        + [pltpu.SemaphoreType.DMA((in_chunks,))] * 2
        + [pltpu.SemaphoreType.DMA((22,))],
        compiler_params=pltpu.CompilerParams(
            collective_id=0, has_side_effects=True, vmem_limit_bytes=24 * 1024 * 1024
        ),
        name="solve",
    )(pltpu.with_memory_space_constraint(points, pltpu.HBM), pltpu.with_memory_space_constraint(modes, pltpu.HBM))
    residual, norms = pl.pallas_call(
        functools.partial(residual_kernel, rows_dev * n),
        out_shape=[
            jax.ShapeDtypeStruct((rows_dev, split), F32),
            jax.ShapeDtypeStruct((steps, split), F32),
        ],
        in_specs=[vmem] * 6,
        out_specs=[hbm, hbm],
        scratch_shapes=[
            pltpu.VMEM((out_chunks, rows_dev // out_chunks, split), F32),
            pltpu.VMEM((steps, split), F32),
            pltpu.SemaphoreType.DMA((out_chunks,)),
            pltpu.SemaphoreType.DMA,
        ],
        compiler_params=pltpu.CompilerParams(vmem_limit_bytes=16 * 1024 * 1024),
        name="residual",
    )(rest, pair, wide, coef, inverse, stat)
    return residual, norms


def solution(mesh):
    axes = tuple((name, mesh.shape[name]) for name in ("rows", "grp"))
    return jax.shard_map(
        functools.partial(on_device, axes),
        mesh=mesh,
        in_specs=(P(("rows", "grp"), None), P()),
        out_specs=(P(("rows", "grp"), None), P()),
        check_vma=False,
    )
```
